256 devices in a mesh: dp: 16 (over y, x), shard: 16 (over z, core).
Axes of the slice: x: 4, y: 4, z: 8, core: 2. Of those that a mesh axis runs over, the one named last changes fastest.
Arguments:
- gradients: bfloat16 [16, 12288, 2048], P('dp', 'shard'), may hold values from -4000 to 4000, as said below
- master_weights: float32 [12288, 2048], P(('shard', 'dp')), may hold values from -6 to 6
- first_moment: float32 [12288, 2048], P(('shard', 'dp')), may hold values from -4 to 4
- second_moment: float32 [12288, 2048], P(('shard', 'dp')), may hold values from 0.05 to 2
Outputs:
- parameters: bfloat16 [12288, 2048], P('shard')
- new_master: float32 [12288, 2048], P(('shard', 'dp'))
- new_first: float32 [12288, 2048], P(('shard', 'dp'))
- new_second: float32 [12288, 2048], P(('shard', 'dp'))
The draws below stay inside these ranges and needn't reach their ends.
Inputs may be any that keep to these rules, and one draw needn't show every extreme that they name: `gradients`: each replica's partial gradient.
All inputs are finite; a program needn't handle non-finite values.
Results may differ from the reference program's by a relative error of at most 0.006.
Values may be sent and summed in bfloat16 or wider, within the bound.
A program may use at most 64 MiB of HBM per device.

```python
import math
import jax
import jax.numpy as jnp
from jax import lax

D = 2048
ROWS_DEV = 48
ROWS = 12288
N_DP = 16


def draw_gradients(key, part):
    keys = jax.random.split(jax.random.fold_in(key, 17), 7)
    shape = (N_DP, ROWS, D)
    groups = ROWS // ROWS_DEV
    group_of_row = jnp.arange(ROWS, dtype=jnp.int32) // ROWS_DEV
    common = jnp.clip(jax.random.normal(keys[5], (1, ROWS, D), jnp.float32), -5.0, 5.0)
    independent = jnp.clip(jax.random.normal(keys[0], shape, jnp.float32), -5.0, 5.0)
    agreement = jax.random.uniform(keys[4], (groups,), jnp.float32, -1.0, 2.0)
    base = independent + agreement[group_of_row][None, :, None] * common
    rise = jnp.arange(ROWS, dtype=jnp.float32) / max(ROWS - 1, 1)
    row_scale = jnp.exp(jax.random.uniform(keys[1], (ROWS,), jnp.float32) * math.log(10.0)) * jnp.exp(rise * math.log(3.0))
    col_scale = jnp.exp(jax.random.uniform(keys[2], (D,), jnp.float32) * math.log(10.0))
    group_keys = jax.random.split(keys[3], groups)
    order = jax.vmap(lambda one_key: jax.random.permutation(one_key, N_DP))(group_keys).astype(jnp.float32)
    rep_table = jnp.exp(order / max(N_DP - 1, 1) * math.log(3.0)) * jnp.exp(jax.random.uniform(keys[6], (groups, N_DP), jnp.float32) * 0.4)
    rep_scale = jnp.transpose(rep_table[group_of_row])
    values = base * row_scale[None, :, None] * col_scale[None, None, :] * rep_scale[:, :, None] * 0.1
    return values.astype(jnp.bfloat16)


def steps_of(own_key, shape, shards, least, top_value):
    level, own = 1.0, jax.random.fold_in(own_key, 6)
    for axis_at, blocks in shards:
        heights = jnp.exp(jax.random.uniform(jax.random.fold_in(own, axis_at), (blocks,), jnp.float32, least / len(shards), top_value / len(shards)))
        level = level * jnp.repeat(heights, shape[axis_at] // blocks).reshape([-1 if axis == axis_at else 1 for axis in range(len(shape))])
    return level


def centred(own_key, dims, scale, bound, shards=(), kind=jnp.bfloat16):
    gain = steps_of(own_key, dims, shards, -0.22, 0.18) if shards else 1.0
    drawn = jax.random.normal(own_key, dims, jnp.float32) * scale * gain
    return jnp.minimum(jnp.maximum(drawn, -bound), bound).astype(kind)


def setup_inputs(seed: int = 0) -> dict:
    key_list = jax.random.split(jax.random.key(seed), 5)
    gradients = draw_gradients(jax.random.fold_in(key_list[4], 71), 0)
    master_weights = centred(key_list[1], (ROWS, D), 1.0, 6.0, ((0, 256),), jnp.float32)
    first_moment = centred(key_list[2], (ROWS, D), 0.3, 4.0, ((0, 256),), jnp.float32)
    second_moment = jnp.clip(jnp.exp(math.log(2.0) - 3.6888794 * jax.random.uniform(key_list[3], (ROWS, D), jnp.float32) ** steps_of(key_list[3], (ROWS, D), ((0, 256),), -0.2, 0.2)), 0.05, 2.0)
    return dict(gradients=gradients, master_weights=master_weights, first_moment=first_moment, second_moment=second_moment)


first_bias = 1.0 - math.exp(100.0 * math.log(0.9))
second_bias = 1.0 - math.exp(100.0 * math.log(0.95))

def adam_update(summed, factor, master_weights, first_moment, second_moment):
    clipped = factor * summed
    new_first = 0.9 * first_moment + 0.1 * clipped
    new_second = 0.95 * second_moment + 0.05 * clipped * clipped
    first_hat = new_first / first_bias
    second_hat = new_second / second_bias
    new_master = master_weights - 0.01 * (first_hat / (jnp.sqrt(second_hat) + 1e-08) + 0.1 * master_weights)
    return (new_master, new_first, new_second)

def reference(gradients, master_weights, first_moment, second_moment):

    def accumulate(total, piece):
        return (total + piece.astype(jnp.float32), None)
    summed, unused = lax.scan(accumulate, jnp.zeros(gradients.shape[1:], jnp.float32), gradients)
    square_sum = jnp.sum(summed * summed)
    limit = 0.5 * math.sqrt(ROWS * D)
    factor = jnp.minimum(1.0, limit / jnp.sqrt(square_sum + 1e-06))
    new_master, new_first, new_second = adam_update(summed, factor, master_weights, first_moment, second_moment)
    parameters = new_master.astype(jnp.bfloat16)
    return (parameters, new_master, new_first, new_second)
```

```python
import math

import jax
import jax.numpy as jnp
from jax import lax
from jax.experimental import pallas as pl
from jax.experimental.pallas import tpu as pltpu
from jax.sharding import Mesh
from jax.sharding import PartitionSpec as P

DP = ("y", "x")
SHARD = ("z", "core")
SHARD_DP = ("z", "core", "y", "x")
MESH = pl.DeviceIdType.MESH

first_bias = 1.0 - math.exp(100.0 * math.log(0.9))
second_bias = 1.0 - math.exp(100.0 * math.log(0.95))

F32 = jnp.float32
BF16 = jnp.bfloat16


class Copies:
    def __init__(self, send_sems, recv_sems):
        self.send_sems, self.recv_sems = send_sems, recv_sems
        self.made = {}

    def start(self, key, src, dst, device):
        at = len(self.made)
        copy = pltpu.make_async_remote_copy(
            src_ref=src,
            dst_ref=dst,
            send_sem=self.send_sems.at[at],
            recv_sem=self.recv_sems.at[at],
            device_id=device,
            device_id_type=MESH,
        )
        copy.start()
        self.made[key] = copy

    def arrived(self, key):
        self.made[key].wait_recv()

    def all_sent(self):
        for copy in self.made.values():
            copy.wait_send()


N_COPIES = 60 + 44 + 30


def kernel(
    entries,
    g_hbm, w_hbm, m_hbm, v_hbm,
    params, w_out, m_out, v_out,
    gv, r1, d1, x1, tf, tb, r2, d2, x2, w, m, v, np_, nz,
    load_sems, send_sems, recv_sems, gossip,
):
    ix, iy = lax.axis_index("x"), lax.axis_index("y")
    iz, ic = lax.axis_index("z"), lax.axis_index("core")
    nz_ring = lax.axis_size("z")
    n_core = lax.axis_size("core")
    half = g_hbm.shape[3] // 2
    quarter = half // 2

    def up(i, by, n=4):
        return lax.rem(i + by, n)

    first_axis, second_axis = ("x", "y"), ("y", "x")
    a = (ix, iy)
    b = (iy, ix)
    step_of = (1, 3)
    group_by = (2, 1, 3, 0)
    cols_of = (pl.ds(0, quarter), pl.ds(quarter, quarter))

    def at_block(ref, h, ai, bi, cols):
        y, x = (bi, ai) if h == 0 else (ai, bi)
        return ref.at[y, x, :, cols]

    def near(axis, i, direction):
        return {axis: up(i, step_of[direction])}

    loads = {}

    def load(key, src, dst):
        copy = pltpu.make_async_copy(src, dst, load_sems.at[len(loads)])
        copy.start()
        loads[key] = copy

    for k in range(4):
        for h in range(2):
            bi = up(b[h], group_by[k])
            cols = pl.ds(h * half, half)
            src = g_hbm.at[bi, :, :, cols] if h == 0 else g_hbm.at[:, bi, :, cols]
            load((h, k), src, gv.at[h, k])
    load("w", w_hbm, w)
    load("m", m_hbm, m)
    load("v", v_hbm, v)

    barrier = pltpu.get_barrier_semaphore()
    neighbours = [{"x": up(ix, s)} for s in step_of] + [{"y": up(iy, s)} for s in step_of]
    neighbours += [{"z": up(iz, s, nz_ring)} for s in (1, nz_ring - 1)]
    neighbours += [{"core": up(ic, s, n_core)} for s in range(1, n_core)]
    for device in neighbours:
        pl.semaphore_signal(barrier, inc=1, device_id=device, device_id_type=MESH)
    pl.semaphore_wait(barrier, len(neighbours))

    rounds = nz_ring // 2

    def tell(r):
        for side, s in enumerate((1, nz_ring - 1)):
            pl.semaphore_signal(
                gossip.at[r, side], inc=1,
                device_id={"z": up(iz, s, nz_ring)}, device_id_type=MESH,
            )

    def told(r):
        for side in range(2):
            pl.semaphore_wait(gossip.at[r, side], 1)

    copies = Copies(send_sems, recv_sems)

    def send_own(k):
        for h in range(2):
            loads[h, k].wait()
            for direction in range(2):
                relayed, other = cols_of[direction], cols_of[1 - direction]
                device = near(first_axis[h], a[h], direction)
                copies.start(
                    ("r1", h, direction, k),
                    gv.at[h, k, up(a[h], 2), :, relayed],
                    r1.at[h, direction, k],
                    device,
                )
            for direction in range(2):
                relayed, other = cols_of[direction], cols_of[1 - direction]
                device = near(first_axis[h], a[h], direction)
                target = up(a[h], step_of[direction])
                copies.start(
                    ("d1o", h, direction, k),
                    gv.at[h, k, target, :, other],
                    d1.at[h, direction, k, :, other],
                    device,
                )

    def relay(k):
        for h in range(2):
            for direction in range(2):
                relayed = cols_of[direction]
                target = up(a[h], step_of[direction])
                copies.arrived(("r1", h, direction, k))
                x1[h, direction, k] = (
                    gv[h, k, target, :, relayed].astype(F32)
                    + r1[h, direction, k].astype(F32)
                ).astype(BF16)
                copies.start(
                    ("d1r", h, direction, k),
                    x1.at[h, direction, k],
                    d1.at[h, direction, k, :, relayed],
                    near(first_axis[h], a[h], direction),
                )

    def complete(k):
        for h in range(2):
            for direction in range(2):
                copies.arrived(("d1o", h, direction, k))
                copies.arrived(("d1r", h, direction, k))
            total = (
                gv[h, k, a[h]].astype(F32)
                + d1[h, 0, k].astype(F32)
                + d1[h, 1, k].astype(F32)
            )
            tf[h, k] = total
            if k < 3:
                tb[h, k] = total.astype(BF16)
            if k == 0:
                for direction in range(2):
                    relayed = cols_of[direction]
                    copies.start(
                        ("r2", h, direction),
                        tb.at[h, 0, :, relayed],
                        r2.at[h, direction],
                        near(second_axis[h], b[h], direction),
                    )
            if k in (1, 2):
                direction = k - 1
                other = cols_of[1 - direction]
                copies.start(
                    ("d2o", h, direction),
                    tb.at[h, k, :, other],
                    d2.at[h, direction, :, other],
                    near(second_axis[h], b[h], direction),
                )

    def relay_second(k):
        direction = k - 1
        relayed = cols_of[direction]
        for h in range(2):
            copies.arrived(("r2", h, direction))
            x2[h, direction] = (
                tf[h, k, :, relayed] + r2[h, direction].astype(F32)
            ).astype(BF16)
            copies.start(
                ("d2r", h, direction),
                x2.at[h, direction],
                d2.at[h, direction, :, relayed],
                near(second_axis[h], b[h], direction),
            )

    send_own(0)
    tell(0)
    send_own(1)
    relay(0)
    told(0)
    tell(1)
    send_own(2)
    relay(1)
    complete(0)
    told(1)
    tell(2)
    send_own(3)
    relay(2)
    complete(1)
    told(2)
    tell(3)
    relay_second(1)
    relay(3)
    complete(2)
    relay_second(2)
    complete(3)
    told(3)

    part = jnp.zeros((8, half), F32)
    for h in range(2):
        for direction in range(2):
            copies.arrived(("d2o", h, direction))
            copies.arrived(("d2r", h, direction))
        total = tf[h, 3] + d2[h, 0].astype(F32) + d2[h, 1].astype(F32)
        tf[h, 3] = total
        square = total * total
        part = part + jnp.sum(square.reshape(-1, 8, half), axis=0)
    row = jnp.sum(part, axis=0, keepdims=True)
    lanes = row[:, 0:128]
    for c in range(1, half // 128):
        lanes = lanes + row[:, c * 128 : (c + 1) * 128]

    np_[0] = lanes
    for i in range(1, 16):
        device = {"y": up(iy, i // 4), "x": up(ix, i % 4)}
        copies.start(("np", i), np_.at[0], np_.at[i], device)
    loads["w"].wait()
    loads["m"].wait()
    loads["v"].wait()
    for i in range(1, 16):
        copies.arrived(("np", i))
    nz[0] = jnp.sum(np_[...], axis=0)
    others = nz_ring * n_core
    for i in range(1, others):
        device = {"z": up(iz, i // n_core, nz_ring), "core": up(ic, i % n_core, n_core)}
        copies.start(("nz", i), nz.at[0], nz.at[i], device)
    for i in range(1, others):
        copies.arrived(("nz", i))
    square_sum = jnp.sum(jnp.sum(nz[...], axis=0), axis=1, keepdims=True)
    limit = 0.5 * math.sqrt(entries)
    factor = jnp.minimum(1.0, limit / jnp.sqrt(square_sum + 1e-06))

    def update(h):
        cols = pl.ds(h * half, half)
        clipped = factor * tf[h, 3]
        new_first = 0.9 * m[:, cols] + 0.1 * clipped
        new_second = 0.95 * v[:, cols] + 0.05 * clipped * clipped
        first_hat = new_first / first_bias
        second_hat = new_second / second_bias
        master = w[:, cols]
        new_master = master - 0.01 * (
            first_hat / (jnp.sqrt(second_hat) + 1e-08) + 0.1 * master
        )
        params[iy, ix, :, cols] = new_master.astype(BF16)
        w_out[:, cols] = new_master
        m_out[:, cols] = new_first
        v_out[:, cols] = new_second

    def columns(h, side=None):
        if side is None:
            return pl.ds(h * half, half)
        return pl.ds(h * half + side * quarter, quarter)

    def along_second(h, direction):
        piece = at_block(params, h, a[h], b[h], columns(h))
        copies.start(("g2", h, direction), piece, piece, near(second_axis[h], b[h], direction))

    def forward_second(h, direction):
        came_from = up(b[h], step_of[1 - direction])
        copies.arrived(("g2", h, direction))
        piece = at_block(params, h, a[h], came_from, columns(h, direction))
        copies.start(("f2", h, direction), piece, piece, near(second_axis[h], b[h], direction))

    def along_first(h, j, side=None):
        bi = up(b[h], (0, 3, 1, 2)[j])
        piece = at_block(params, h, a[h], bi, columns(h, side))
        for direction in range(2):
            copies.start(
                ("g1", h, direction, j, side), piece, piece,
                near(first_axis[h], a[h], direction),
            )

    def forward_first(h, j):
        bi = up(b[h], (0, 3, 1, 2)[j])
        for direction in range(2):
            side = direction if j == 3 else None
            copies.arrived(("g1", h, direction, j, side))
            came_from = up(a[h], step_of[1 - direction])
            piece = at_block(params, h, came_from, bi, columns(h, direction))
            copies.start(
                ("f1", h, direction, j), piece, piece,
                near(first_axis[h], a[h], direction),
            )

    for h in range(2):
        update(h)
        for direction in range(2):
            along_second(h, direction)
    for h in range(2):
        along_first(h, 0)
    for j in (1, 2):
        for h in range(2):
            forward_second(h, j - 1)
            along_first(h, j)
    for h in range(2):
        forward_first(h, 0)
    for direction in range(2):
        for h in range(2):
            copies.arrived(("f2", h, direction))
            along_first(h, 3, direction)
    for j in (1, 2, 3):
        for h in range(2):
            forward_first(h, j)
    for h in range(2):
        for direction in range(2):
            copies.arrived(("g1", h, direction, 3, 1 - direction))
            for j in range(4):
                copies.arrived(("f1", h, direction, j))
    copies.all_sent()


def per_device(gradients, master_weights, first_moment, second_moment):
    rows, width = master_weights.shape
    entries = rows * lax.axis_size(DP) * lax.axis_size(SHARD) * width
    half, quarter = width // 2, width // 4
    grads = gradients.reshape(4, 4, rows, width)
    owned = jax.ShapeDtypeStruct((rows, width), F32)
    hbm = pl.BlockSpec(memory_space=pltpu.HBM)
    vmem = pl.BlockSpec(memory_space=pltpu.VMEM)
    peers = lax.axis_size("z") * lax.axis_size("core")
    parameters, new_master, new_first, new_second = pl.pallas_call(
        lambda *refs: kernel(entries, *refs),
        out_shape=(jax.ShapeDtypeStruct((4, 4, rows, width), BF16), owned, owned, owned),
        in_specs=[hbm] * 4,
        out_specs=(vmem,) * 4,
        scratch_shapes=[
            pltpu.VMEM((2, 4, 4, rows, half), BF16),
            pltpu.VMEM((2, 2, 4, rows, quarter), BF16),
            pltpu.VMEM((2, 2, 4, rows, half), BF16),
            pltpu.VMEM((2, 2, 4, rows, quarter), BF16),
            pltpu.VMEM((2, 4, rows, half), F32),
            pltpu.VMEM((2, 3, rows, half), BF16),
            pltpu.VMEM((2, 2, rows, quarter), BF16),
            pltpu.VMEM((2, 2, rows, half), BF16),
            pltpu.VMEM((2, 2, rows, quarter), BF16),
            pltpu.VMEM((rows, width), F32),
            pltpu.VMEM((rows, width), F32),
            pltpu.VMEM((rows, width), F32),
            pltpu.VMEM((16, 1, 128), F32),
            pltpu.VMEM((peers, 1, 128), F32),
            pltpu.SemaphoreType.DMA((11,)),
            pltpu.SemaphoreType.DMA((N_COPIES,)),
            pltpu.SemaphoreType.DMA((N_COPIES,)),
            pltpu.SemaphoreType.REGULAR((lax.axis_size("z") // 2, 2)),
        ],
        compiler_params=pltpu.CompilerParams(collective_id=0, has_side_effects=True),
    )(grads, master_weights, first_moment, second_moment)
    return (parameters.reshape(16 * rows, width), new_master, new_first, new_second)


def solution(mesh):
    split = Mesh(mesh.devices.reshape(4, 4, 8, 2), ("y", "x", "z", "core"))
    return jax.shard_map(
        per_device,
        mesh=split,
        in_specs=(P(DP, SHARD, None), P(SHARD_DP, None), P(SHARD_DP, None), P(SHARD_DP, None)),
        out_specs=(P(SHARD, None), P(SHARD_DP, None), P(SHARD_DP, None), P(SHARD_DP, None)),
        check_vma=False,
    )
```

```python
import math

import jax
import jax.numpy as jnp
from jax import lax
from jax.experimental import pallas as pl
from jax.experimental.pallas import tpu as pltpu
from jax.sharding import Mesh
from jax.sharding import PartitionSpec as P

DP = ("y", "x")
SHARD = ("z", "core")
SHARD_DP = ("z", "core", "y", "x")
MESH = pl.DeviceIdType.MESH

first_bias = 1.0 - math.exp(100.0 * math.log(0.9))
second_bias = 1.0 - math.exp(100.0 * math.log(0.95))

F32 = jnp.float32
BF16 = jnp.bfloat16


class Copies:
    def __init__(self, send_sems, recv_sems):
        self.send_sems, self.recv_sems = send_sems, recv_sems
        self.made = {}

    def start(self, key, src, dst, device):
        at = len(self.made)
        copy = pltpu.make_async_remote_copy(
            src_ref=src,
            dst_ref=dst,
            send_sem=self.send_sems.at[at],
            recv_sem=self.recv_sems.at[at],
            device_id=device,
            device_id_type=MESH,
        )
        copy.start()
        self.made[key] = copy

    def arrived(self, key):
        self.made[key].wait_recv()

    def all_sent(self):
        for copy in self.made.values():
            copy.wait_send()


VMEM_LIMIT = 59 * 2**20

N_COPIES = 60 + 44 + 30


def kernel(
    entries,
    g_hbm, w_hbm, m_hbm, v_hbm,
    params, w_out, m_out, v_out,
    gv, r1, d1, x1, tf, tb, r2, d2, x2, w, m, v, np_, nz,
    load_sems, send_sems, recv_sems, gossip,
):
    ix, iy = lax.axis_index("x"), lax.axis_index("y")
    iz, ic = lax.axis_index("z"), lax.axis_index("core")
    nz_ring = lax.axis_size("z")
    n_core = lax.axis_size("core")
    half = g_hbm.shape[3] // 2
    quarter = half // 2

    def up(i, by, n=4):
        return lax.rem(i + by, n)

    first_axis, second_axis = ("x", "y"), ("y", "x")
    a = (ix, iy)
    b = (iy, ix)
    step_of = (1, 3)
    group_by = (2, 1, 3, 0)
    cols_of = (pl.ds(0, quarter), pl.ds(quarter, quarter))

    def at_block(ref, h, ai, bi, cols):
        y, x = (bi, ai) if h == 0 else (ai, bi)
        return ref.at[y, x, :, cols]

    def near(axis, i, direction):
        return {axis: up(i, step_of[direction])}

    loads = {}

    def load(key, src, dst):
        copy = pltpu.make_async_copy(src, dst, load_sems.at[len(loads)])
        copy.start()
        loads[key] = copy

    for k in range(4):
        for h in range(2):
            bi = up(b[h], group_by[k])
            cols = pl.ds(h * half, half)
            src = g_hbm.at[bi, :, :, cols] if h == 0 else g_hbm.at[:, bi, :, cols]
            load((h, k), src, gv.at[h, k])
    load("w", w_hbm, w)
    load("m", m_hbm, m)
    load("v", v_hbm, v)

    barrier = pltpu.get_barrier_semaphore()
    neighbours = [{"x": up(ix, s)} for s in step_of] + [{"y": up(iy, s)} for s in step_of]
    neighbours += [{"z": up(iz, s, nz_ring)} for s in (1, nz_ring - 1)]
    neighbours += [{"core": up(ic, s, n_core)} for s in range(1, n_core)]
    for device in neighbours:
        pl.semaphore_signal(barrier, inc=1, device_id=device, device_id_type=MESH)
    pl.semaphore_wait(barrier, len(neighbours))

    rounds = nz_ring // 2

    def tell(r):
        for side, s in enumerate((1, nz_ring - 1)):
            pl.semaphore_signal(
                gossip.at[r, side], inc=1,
                device_id={"z": up(iz, s, nz_ring)}, device_id_type=MESH,
            )

    def told(r):
        for side in range(2):
            pl.semaphore_wait(gossip.at[r, side], 1)

    copies = Copies(send_sems, recv_sems)

    def send_own(k):
        for h in range(2):
            loads[h, k].wait()
            for direction in range(2):
                relayed, other = cols_of[direction], cols_of[1 - direction]
                device = near(first_axis[h], a[h], direction)
                copies.start(
                    ("r1", h, direction, k),
                    gv.at[h, k, up(a[h], 2), :, relayed],
                    r1.at[h, direction, k],
                    device,
                )
            for direction in range(2):
                relayed, other = cols_of[direction], cols_of[1 - direction]
                device = near(first_axis[h], a[h], direction)
                target = up(a[h], step_of[direction])
                copies.start(
                    ("d1o", h, direction, k),
                    gv.at[h, k, target, :, other],
                    d1.at[h, direction, k, :, other],
                    device,
                )

    def relay(k):
        for h in range(2):
            for direction in range(2):
                relayed = cols_of[direction]
                target = up(a[h], step_of[direction])
                copies.arrived(("r1", h, direction, k))
                x1[h, direction, k] = (
                    gv[h, k, target, :, relayed].astype(F32)
                    + r1[h, direction, k].astype(F32)
                ).astype(BF16)
                copies.start(
                    ("d1r", h, direction, k),
                    x1.at[h, direction, k],
                    d1.at[h, direction, k, :, relayed],
                    near(first_axis[h], a[h], direction),
                )

    def complete(k):
        for h in range(2):
            for direction in range(2):
                copies.arrived(("d1o", h, direction, k))
                copies.arrived(("d1r", h, direction, k))
            total = (
                gv[h, k, a[h]].astype(F32)
                + d1[h, 0, k].astype(F32)
                + d1[h, 1, k].astype(F32)
            )
            tf[h, k] = total
            if k < 3:
                tb[h, k] = total.astype(BF16)
            if k == 0:
                for direction in range(2):
                    relayed = cols_of[direction]
                    copies.start(
                        ("r2", h, direction),
                        tb.at[h, 0, :, relayed],
                        r2.at[h, direction],
                        near(second_axis[h], b[h], direction),
                    )
            if k in (1, 2):
                direction = k - 1
                other = cols_of[1 - direction]
                copies.start(
                    ("d2o", h, direction),
                    tb.at[h, k, :, other],
                    d2.at[h, direction, :, other],
                    near(second_axis[h], b[h], direction),
                )

    def relay_second(k):
        direction = k - 1
        relayed = cols_of[direction]
        for h in range(2):
            copies.arrived(("r2", h, direction))
            x2[h, direction] = (
                tf[h, k, :, relayed] + r2[h, direction].astype(F32)
            ).astype(BF16)
            copies.start(
                ("d2r", h, direction),
                x2.at[h, direction],
                d2.at[h, direction, :, relayed],
                near(second_axis[h], b[h], direction),
            )

    send_own(0)
    tell(0)
    send_own(1)
    relay(0)
    told(0)
    tell(1)
    send_own(2)
    relay(1)
    complete(0)
    told(1)
    tell(2)
    send_own(3)
    relay(2)
    complete(1)
    told(2)
    tell(3)
    relay_second(1)
    relay(3)
    complete(2)
    relay_second(2)
    complete(3)
    told(3)

    part = jnp.zeros((8, half), F32)
    for h in range(2):
        for direction in range(2):
            copies.arrived(("d2o", h, direction))
            copies.arrived(("d2r", h, direction))
        total = tf[h, 3] + d2[h, 0].astype(F32) + d2[h, 1].astype(F32)
        tf[h, 3] = total
        square = total * total
        part = part + jnp.sum(square.reshape(-1, 8, half), axis=0)
    row = jnp.sum(part, axis=0, keepdims=True)
    lanes = row[:, 0:128]
    for c in range(1, half // 128):
        lanes = lanes + row[:, c * 128 : (c + 1) * 128]

    np_[0] = lanes
    for i in range(1, 16):
        device = {"y": up(iy, i // 4), "x": up(ix, i % 4)}
        copies.start(("np", i), np_.at[0], np_.at[i], device)
    loads["w"].wait()
    loads["m"].wait()
    loads["v"].wait()
    for i in range(1, 16):
        copies.arrived(("np", i))
    nz[0] = jnp.sum(np_[...], axis=0)
    others = nz_ring * n_core
    for i in range(1, others):
        device = {"z": up(iz, i // n_core, nz_ring), "core": up(ic, i % n_core, n_core)}
        copies.start(("nz", i), nz.at[0], nz.at[i], device)
    for i in range(1, others):
        copies.arrived(("nz", i))
    square_sum = jnp.sum(jnp.sum(nz[...], axis=0), axis=1, keepdims=True)
    limit = 0.5 * math.sqrt(entries)
    factor = jnp.minimum(1.0, limit / jnp.sqrt(square_sum + 1e-06))

    def update(h):
        cols = pl.ds(h * half, half)
        clipped = factor * tf[h, 3]
        new_first = 0.9 * m[:, cols] + 0.1 * clipped
        new_second = 0.95 * v[:, cols] + 0.05 * clipped * clipped
        first_hat = new_first / first_bias
        second_hat = new_second / second_bias
        master = w[:, cols]
        new_master = master - 0.01 * (
            first_hat / (jnp.sqrt(second_hat) + 1e-08) + 0.1 * master
        )
        params[iy, ix, :, cols] = new_master.astype(BF16)
        w_out[:, cols] = new_master
        m_out[:, cols] = new_first
        v_out[:, cols] = new_second

    def columns(h, side=None):
        if side is None:
            return pl.ds(h * half, half)
        return pl.ds(h * half + side * quarter, quarter)

    def along_second(h, direction):
        piece = at_block(params, h, a[h], b[h], columns(h))
        copies.start(("g2", h, direction), piece, piece, near(second_axis[h], b[h], direction))

    def forward_second(h, direction):
        came_from = up(b[h], step_of[1 - direction])
        copies.arrived(("g2", h, direction))
        piece = at_block(params, h, a[h], came_from, columns(h, direction))
        copies.start(("f2", h, direction), piece, piece, near(second_axis[h], b[h], direction))

    def along_first(h, j, side=None):
        bi = up(b[h], (0, 3, 1, 2)[j])
        piece = at_block(params, h, a[h], bi, columns(h, side))
        for direction in range(2):
            copies.start(
                ("g1", h, direction, j, side), piece, piece,
                near(first_axis[h], a[h], direction),
            )

    def forward_first(h, j):
        bi = up(b[h], (0, 3, 1, 2)[j])
        for direction in range(2):
            side = direction if j == 3 else None
            copies.arrived(("g1", h, direction, j, side))
            came_from = up(a[h], step_of[1 - direction])
            piece = at_block(params, h, came_from, bi, columns(h, direction))
            copies.start(
                ("f1", h, direction, j), piece, piece,
                near(first_axis[h], a[h], direction),
            )

    for h in range(2):
        update(h)
        for direction in range(2):
            along_second(h, direction)
    for h in range(2):
        along_first(h, 0)
    for j in (1, 2):
        for h in range(2):
            forward_second(h, j - 1)
            along_first(h, j)
    for h in range(2):
        forward_first(h, 0)
    for direction in range(2):
        for h in range(2):
            copies.arrived(("f2", h, direction))
            along_first(h, 3, direction)
    for j in (1, 2, 3):
        for h in range(2):
            forward_first(h, j)
    for h in range(2):
        for direction in range(2):
            copies.arrived(("g1", h, direction, 3, 1 - direction))
            for j in range(4):
                copies.arrived(("f1", h, direction, j))
    copies.all_sent()


def per_device(gradients, master_weights, first_moment, second_moment):
    rows, width = master_weights.shape
    entries = rows * lax.axis_size(DP) * lax.axis_size(SHARD) * width
    half, quarter = width // 2, width // 4
    grads = gradients.reshape(4, 4, rows, width)
    owned = pltpu.VMEM((rows, width), F32)
    hbm = pl.BlockSpec(memory_space=pltpu.HBM)
    vmem = pl.BlockSpec(memory_space=pltpu.VMEM)
    peers = lax.axis_size("z") * lax.axis_size("core")
    parameters, new_master, new_first, new_second = pl.pallas_call(
        lambda *refs: kernel(entries, *refs),
        out_shape=(pltpu.VMEM((4, 4, rows, width), BF16), owned, owned, owned),
        in_specs=[hbm] * 4,
        out_specs=(vmem,) * 4,
        scratch_shapes=[
            pltpu.VMEM((2, 4, 4, rows, half), BF16),
            pltpu.VMEM((2, 2, 4, rows, quarter), BF16),
            pltpu.VMEM((2, 2, 4, rows, half), BF16),
            pltpu.VMEM((2, 2, 4, rows, quarter), BF16),
            pltpu.VMEM((2, 4, rows, half), F32),
            pltpu.VMEM((2, 3, rows, half), BF16),
            pltpu.VMEM((2, 2, rows, quarter), BF16),
            pltpu.VMEM((2, 2, rows, half), BF16),
            pltpu.VMEM((2, 2, rows, quarter), BF16),
            pltpu.VMEM((rows, width), F32),
            pltpu.VMEM((rows, width), F32),
            pltpu.VMEM((rows, width), F32),
            pltpu.VMEM((16, 1, 128), F32),
            pltpu.VMEM((peers, 1, 128), F32),
            pltpu.SemaphoreType.DMA((11,)),
            pltpu.SemaphoreType.DMA((N_COPIES,)),
            pltpu.SemaphoreType.DMA((N_COPIES,)),
            pltpu.SemaphoreType.REGULAR((lax.axis_size("z") // 2, 2)),
        ],
        compiler_params=pltpu.CompilerParams(
            collective_id=0, has_side_effects=True, vmem_limit_bytes=VMEM_LIMIT
        ),
    )(grads, master_weights, first_moment, second_moment)
    return (parameters.reshape(16 * rows, width), new_master, new_first, new_second)


def solution(mesh):
    split = Mesh(mesh.devices.reshape(4, 4, 8, 2), ("y", "x", "z", "core"))
    return jax.shard_map(
        per_device,
        mesh=split,
        in_specs=(P(DP, SHARD, None), P(SHARD_DP, None), P(SHARD_DP, None), P(SHARD_DP, None)),
        out_specs=(P(SHARD, None), P(SHARD_DP, None), P(SHARD_DP, None), P(SHARD_DP, None)),
        check_vma=False,
    )
```

```python
import math

import jax
import jax.numpy as jnp
from jax import lax
from jax.experimental import pallas as pl
from jax.experimental.pallas import tpu as pltpu
from jax.sharding import Mesh
from jax.sharding import PartitionSpec as P

DP = ("y", "x")
SHARD = ("z", "core")
SHARD_DP = ("z", "core", "y", "x")
MESH = pl.DeviceIdType.MESH

first_bias = 1.0 - math.exp(100.0 * math.log(0.9))
second_bias = 1.0 - math.exp(100.0 * math.log(0.95))

F32 = jnp.float32
BF16 = jnp.bfloat16
VMEM_LIMIT = 59 * 2**20


def table(*groups):
    keys = []
    for name, *dims in groups:
        index = [()]
        for dim in dims:
            index = [i + (j,) for i in index for j in range(dim)]
        keys += [(name, *i) for i in index]
    return {key: at for at, key in enumerate(keys)}


RECEIVED = table(
    ("r1", 2, 4), ("d1", 2, 4), ("r2", 2), ("d2", 2), ("np",), ("nz",),
    ("g2", 2, 2, 2), ("f2", 2, 2), ("g1", 2, 4, 2), ("f1",),
)
SENT = table(("rs",), ("np",), ("nz",), ("ag",))
LOADED = table(("gx", 2), ("gv", 2), ("state",))


def kernel(
    entries,
    g_hbm, w_hbm, m_hbm, v_hbm,
    params, w_out, m_out, v_out,
    gx, gv, land, x1, tf, tb, x2, state, np_, nz,
    load_sems, send_sems, recv_sems, gossip,
):
    ix, iy = lax.axis_index("x"), lax.axis_index("y")
    iz, ic = lax.axis_index("z"), lax.axis_index("core")
    z_size = lax.axis_size("z")
    n_core = lax.axis_size("core")
    half = g_hbm.shape[3] // 2
    quarter = half // 2

    def up(i, by, n=4):
        return lax.rem(i + by, n)

    first_axis, second_axis = ("x", "y"), ("y", "x")
    a = (ix, iy)
    b = (iy, ix)
    step_of = (1, 3)
    group_by = (2, 1, 3, 0)

    def r1(h, k):
        return land.at[pl.ds((h * 4 + k) * 2, 2)]

    def d1(h, k):
        return land.at[pl.ds(16 + (h * 4 + k) * 4, 4)]

    def r2(h):
        return land.at[pl.ds(48 + h * 2, 2)]

    def d2(h):
        return land.at[pl.ds(52 + h * 4, 4)]

    def whole(ref, direction):
        return jnp.concatenate(
            [ref[direction * 2].astype(F32), ref[direction * 2 + 1].astype(F32)], axis=1
        )

    def cols(h, side=None):
        if side is None:
            return pl.ds(h * half, half)
        return pl.ds(h * half + side * quarter, quarter)

    def side_cols(side):
        return pl.ds(side * quarter, quarter)

    def block(h, ai, bi):
        return (bi, ai) if h == 0 else (ai, bi)

    def near(axis, i, direction):
        return {axis: up(i, step_of[direction])}

    def along_first(h, direction):
        return near(first_axis[h], a[h], direction)

    def along_second(h, direction):
        return near(second_axis[h], b[h], direction)

    def load(key, src, dst):
        pltpu.make_async_copy(src, dst, load_sems.at[LOADED[key]]).start()

    def loaded(key, dst):
        pltpu.make_async_copy(dst, dst, load_sems.at[LOADED[key]]).wait()

    for h in range(2):
        far = up(a[h], 2)
        src = g_hbm.at[:, far, :, cols(h)] if h == 0 else g_hbm.at[far, :, :, cols(h)]
        load(("gx", h), src, gx.at[h])

    barrier = pltpu.get_barrier_semaphore()
    neighbours = [{"x": up(ix, s)} for s in step_of] + [{"y": up(iy, s)} for s in step_of]
    neighbours += [{"z": up(iz, s, z_size)} for s in (1, z_size - 1)]
    neighbours += [{"core": up(ic, s, n_core)} for s in range(1, n_core)]
    for device in neighbours:
        pl.semaphore_signal(barrier, inc=1, device_id=device, device_id_type=MESH)

    for h in range(2):
        load(("gv", h), g_hbm.at[:, :, :, cols(h)], gv.at[h])
    for i, ref in enumerate((w_hbm, m_hbm, v_hbm)):
        load(("state",), ref, state.at[i])
    pl.semaphore_wait(barrier, len(neighbours))

    def tell(r):
        for s in (1, z_size - 1):
            pl.semaphore_signal(
                gossip.at[r], inc=1,
                device_id={"z": up(iz, s, z_size)}, device_id_type=MESH,
            )

    def told(r):
        pl.semaphore_wait(gossip.at[r], 2)

    def send(sent, key, src, dst, device):
        pltpu.make_async_remote_copy(
            src_ref=src,
            dst_ref=dst,
            send_sem=send_sems.at[SENT[sent,]],
            recv_sem=recv_sems.at[RECEIVED[key]],
            device_id=device,
            device_id_type=MESH,
        ).start()

    def arrived(key, bytes_of):
        pltpu.make_async_copy(bytes_of, bytes_of, recv_sems.at[RECEIVED[key]]).wait()

    def all_sent(sent, bytes_of):
        pltpu.make_async_copy(bytes_of, bytes_of, send_sems.at[SENT[sent,]]).wait()

    def send_far(k):
        for h in range(2):
            bi = up(b[h], group_by[k])
            for direction in range(2):
                send(
                    "rs", ("r1", h, k),
                    gx.at[h, bi, :, side_cols(direction)],
                    r1(h, k).at[direction],
                    along_first(h, direction),
                )

    def send_near(k):
        for h in range(2):
            bi = up(b[h], group_by[k])
            for direction in range(2):
                other = 1 - direction
                y, x = block(h, up(a[h], step_of[direction]), bi)
                send(
                    "rs", ("d1", h, k),
                    gv.at[h, y, x, :, side_cols(other)],
                    d1(h, k).at[direction * 2 + other],
                    along_first(h, direction),
                )

    def relay(k):
        for h in range(2):
            bi = up(b[h], group_by[k])
            arrived(("r1", h, k), r1(h, k))
            for direction in range(2):
                y, x = block(h, up(a[h], step_of[direction]), bi)
                x1[h, k, direction] = (
                    gv[h, y, x, :, side_cols(direction)].astype(F32)
                    + r1(h, k)[direction].astype(F32)
                ).astype(BF16)
                send(
                    "rs", ("d1", h, k),
                    x1.at[h, k, direction],
                    d1(h, k).at[direction * 2 + direction],
                    along_first(h, direction),
                )

    def complete(k):
        for h in range(2):
            bi = up(b[h], group_by[k])
            arrived(("d1", h, k), d1(h, k))
            y, x = block(h, a[h], bi)
            total = gv[h, y, x].astype(F32) + whole(d1(h, k), 0) + whole(d1(h, k), 1)
            tf[h, k] = total
            if k < 3:
                tb[h, k] = total.astype(BF16)
            if k == 0:
                for direction in range(2):
                    send(
                        "rs", ("r2", h),
                        tb.at[h, 0, :, side_cols(direction)],
                        r2(h).at[direction],
                        along_second(h, direction),
                    )
            if k in (1, 2):
                direction = k - 1
                other = 1 - direction
                send(
                    "rs", ("d2", h),
                    tb.at[h, k, :, side_cols(other)],
                    d2(h).at[direction * 2 + other],
                    along_second(h, direction),
                )

    def relay_second():
        for h in range(2):
            arrived(("r2", h), r2(h))
            for direction in range(2):
                x2[h, direction] = (
                    tf[h, 1 + direction, :, side_cols(direction)]
                    + r2(h)[direction].astype(F32)
                ).astype(BF16)
                send(
                    "rs", ("d2", h),
                    x2.at[h, direction],
                    d2(h).at[direction * 2 + direction],
                    along_second(h, direction),
                )

    for h in range(2):
        loaded(("gx", h), gx.at[h])
    for k in range(4):
        send_far(k)
    tell(0)
    for h in range(2):
        loaded(("gv", h), gv.at[h])
    send_near(0)
    relay(0)
    told(0)
    tell(1)
    send_near(1)
    relay(1)
    relay(2)
    told(1)
    tell(2)
    send_near(2)
    complete(0)
    relay(3)
    told(2)
    tell(3)
    complete(1)
    send_near(3)
    complete(2)
    relay_second()
    complete(3)
    told(3)
    loaded(("state",), state)

    lanes = jnp.zeros((8, 128), F32)
    for h in range(2):
        arrived(("d2", h), d2(h))
        total = tf[h, 3] + whole(d2(h), 0) + whole(d2(h), 1)
        tf[h, 3] = total
        square = total * total
        by_row = jnp.sum(square.reshape(-1, 8, half), axis=0)
        for c in range(half // 128):
            lanes = lanes + by_row[:, c * 128 : (c + 1) * 128]

    np_[0] = jnp.sum(lanes, axis=0, keepdims=True)
    distance = {0: 0, 1: 1, 2: 2, 3: 1}
    plane = sorted(
        ((i, j) for i in range(4) for j in range(4)),
        key=lambda at: -distance[at[0]] - distance[at[1]],
    )[:-1]
    for i, j in plane:
        slot = i * 4 + j
        send("np", ("np",), np_.at[0], np_.at[slot], {"y": up(iy, i), "x": up(ix, j)})
    arrived(("np",), np_.at[pl.ds(1, 15)])
    nz[0] = jnp.sum(np_[...], axis=0)
    line = sorted(
        ((i, j) for i in range(z_size) for j in range(n_core)),
        key=lambda at: -min(at[0], z_size - at[0]) - 0.5 * at[1],
    )[:-1]
    for i, j in line:
        slot = i * n_core + j
        device = {"z": up(iz, i, z_size), "core": up(ic, j, n_core)}
        send("nz", ("nz",), nz.at[0], nz.at[slot], device)
    arrived(("nz",), nz.at[pl.ds(1, len(line))])
    square_sum = jnp.sum(jnp.sum(nz[...], axis=0), axis=1, keepdims=True)
    limit = 0.5 * math.sqrt(entries)
    factor = jnp.minimum(1.0, limit / jnp.sqrt(square_sum + 1e-06))

    def update(h):
        at = cols(h)
        clipped = factor * tf[h, 3]
        new_first = 0.9 * state[1, :, at] + 0.1 * clipped
        new_second = 0.95 * state[2, :, at] + 0.05 * clipped * clipped
        first_hat = new_first * (1.0 / first_bias)
        second_hat = new_second * (1.0 / second_bias)
        master = state[0, :, at]
        new_master = master - 0.01 * (
            first_hat / (jnp.sqrt(second_hat) + 1e-08) + 0.1 * master
        )
        params[iy, ix, :, at] = new_master.astype(BF16)
        w_out[:, at] = new_master
        m_out[:, at] = new_first
        v_out[:, at] = new_second

    def piece(h, ai, bi, side):
        y, x = block(h, ai, bi)
        return params.at[y, x, :, cols(h, side)]

    arrived_from = (0, 3, 1, 2)

    def gather_second(relayed, halves):
        for h in halves:
            for direction in range(2):
                side = direction if relayed else 1 - direction
                part = piece(h, a[h], b[h], side)
                send("ag", ("g2", h, direction, side), part, part, along_second(h, direction))

    def forward_second(direction):
        for h in range(2):
            arrived(("g2", h, direction, direction), x2.at[0, 0])
            part = piece(h, a[h], up(b[h], step_of[1 - direction]), direction)
            send("ag", ("f2", h, direction), part, part, along_second(h, direction))

    def gather_first(j, side):
        for h in range(2):
            if j in (1, 2):
                if side != j - 1:
                    arrived(("g2", h, j - 1, side), x2.at[0, 0])
            if j == 3:
                arrived(("f2", h, side), x2.at[0, 0])
            part = piece(h, a[h], up(b[h], arrived_from[j]), side)
            for direction in range(2):
                send("ag", ("g1", h, j, side), part, part, along_first(h, direction))

    def forward_first(j, direction):
        for h in range(2):
            arrived(("g1", h, j, direction), x2.at[0])
            came_from = up(a[h], step_of[1 - direction])
            part = piece(h, came_from, up(b[h], arrived_from[j]), direction)
            send("ag", ("f1",), part, part, along_first(h, direction))

    for h in range(2):
        update(h)
        gather_second(True, (h,))
    gather_first(0, 0)
    gather_first(0, 1)
    gather_second(False, (0, 1))
    forward_second(0)
    gather_first(1, 0)
    forward_second(1)
    gather_first(2, 1)
    gather_first(1, 1)
    gather_first(3, 0)
    gather_first(2, 0)
    forward_first(1, 0)
    gather_first(3, 1)
    forward_first(0, 1)
    forward_first(0, 0)
    forward_first(1, 1)
    forward_first(2, 0)
    forward_first(2, 1)
    forward_first(3, 0)
    forward_first(3, 1)
    all_sent("rs", land)
    all_sent("np", np_.at[pl.ds(1, 15)])
    all_sent("nz", nz.at[pl.ds(1, len(line))])
    arrived(("f1",), x1)
    all_sent("ag", land)


def write_out(*refs):
    n = (len(refs) - 1) // 2
    sources, targets, sems = refs[:n], refs[n : 2 * n], refs[-1]
    copies = []
    for src, dst in zip(sources, targets):
        parts = [(src.at[i], dst.at[i]) for i in range(4)] if len(src.shape) == 4 else [(src, dst)]
        copies += parts
    made = [
        pltpu.make_async_copy(src, dst, sems.at[i]) for i, (src, dst) in enumerate(copies)
    ]
    for copy in made:
        copy.start()
    for copy in made:
        copy.wait()


def per_device(gradients, master_weights, first_moment, second_moment):
    rows, width = master_weights.shape
    entries = rows * lax.axis_size(DP) * lax.axis_size(SHARD) * width
    half, quarter = width // 2, width // 4
    grads = gradients.reshape(4, 4, rows, width)
    shapes = [((4, 4, rows, width), BF16)] + [((rows, width), F32)] * 3
    hbm = pl.BlockSpec(memory_space=pltpu.HBM)
    vmem = pl.BlockSpec(memory_space=pltpu.VMEM)
    z_size = lax.axis_size("z")
    results = pl.pallas_call(
        lambda *refs: kernel(entries, *refs),
        out_shape=[pltpu.VMEM(*shape) for shape in shapes],
        in_specs=[hbm] * 4,
        out_specs=[vmem] * 4,
        scratch_shapes=[
            pltpu.VMEM((2, 4, rows, half), BF16),
            pltpu.VMEM((2, 4, 4, rows, half), BF16),
            pltpu.VMEM((60, rows, quarter), BF16),
            pltpu.VMEM((2, 4, 2, rows, quarter), BF16),
            pltpu.VMEM((2, 4, rows, half), F32),
            pltpu.VMEM((2, 3, rows, half), BF16),
            pltpu.VMEM((2, 2, rows, quarter), BF16),
            pltpu.VMEM((3, rows, width), F32),
            pltpu.VMEM((16, 1, 128), F32),
            pltpu.VMEM((z_size * lax.axis_size("core"), 1, 128), F32),
            pltpu.SemaphoreType.DMA((len(LOADED),)),
            pltpu.SemaphoreType.DMA((len(SENT),)),
            pltpu.SemaphoreType.DMA((len(RECEIVED),)),
            pltpu.SemaphoreType.REGULAR((z_size // 2,)),
        ],
        compiler_params=pltpu.CompilerParams(
            collective_id=0, has_side_effects=True, vmem_limit_bytes=VMEM_LIMIT
        ),
    )(grads, master_weights, first_moment, second_moment)
    parameters, new_master, new_first, new_second = pl.pallas_call(
        write_out,
        out_shape=[jax.ShapeDtypeStruct(*shape) for shape in shapes],
        in_specs=[vmem] * 4,
        out_specs=[hbm] * 4,
        scratch_shapes=[pltpu.SemaphoreType.DMA((7,))],
        compiler_params=pltpu.CompilerParams(vmem_limit_bytes=2**20),
    )(*results)
    return (parameters.reshape(16 * rows, width), new_master, new_first, new_second)


def solution(mesh):
    split = Mesh(mesh.devices.reshape(4, 4, 8, 2), ("y", "x", "z", "core"))
    return jax.shard_map(
        per_device,
        mesh=split,
        in_specs=(P(DP, SHARD, None), P(SHARD_DP, None), P(SHARD_DP, None), P(SHARD_DP, None)),
        out_specs=(P(SHARD, None), P(SHARD_DP, None), P(SHARD_DP, None), P(SHARD_DP, None)),
        check_vma=False,
    )
```

```python
import math

import jax
import jax.numpy as jnp
from jax import lax
from jax.experimental import pallas as pl
from jax.experimental.pallas import tpu as pltpu
from jax.sharding import Mesh
from jax.sharding import PartitionSpec as P

DP = ("y", "x")
SHARD = ("z", "core")
SHARD_DP = ("z", "core", "y", "x")
MESH = pl.DeviceIdType.MESH

first_bias = 1.0 - math.exp(100.0 * math.log(0.9))
second_bias = 1.0 - math.exp(100.0 * math.log(0.95))

F32 = jnp.float32
BF16 = jnp.bfloat16
VMEM_LIMIT = 59 * 2**20


def table(*groups):
    keys = []
    for name, *dims in groups:
        index = [()]
        for dim in dims:
            index = [i + (j,) for i in index for j in range(dim)]
        keys += [(name, *i) for i in index]
    return {key: at for at, key in enumerate(keys)}


NORM = table(("np",), ("nz",))
REDUCE = table(*NORM, ("r1", 4), ("d1", 4), ("r2",), ("d2",))
GATHER = table(*NORM, ("g2", 2, 2), ("f2", 2), ("g1", 4, 2), ("f1",))
RECEIVED = {**REDUCE, **GATHER}
N_RECEIVED = max(len(REDUCE), len(GATHER))
SENT = table(("rs",), ("np",), ("nz",), ("ag",))
LOADED = table(("gx",), ("gv",), ("state",))


def kernel(
    entries,
    g_hbm, w_hbm, m_hbm, v_hbm,
    params, w_out, m_out, v_out,
    gx, gv, land, x1, tf, tb, x2, state, np_, nz,
    load_sems, send_sems, recv_sems, gossip,
):
    ix, iy = lax.axis_index("x"), lax.axis_index("y")
    iz, ic = lax.axis_index("z"), lax.axis_index("core")
    z_size = lax.axis_size("z")
    n_core = lax.axis_size("core")
    half = g_hbm.shape[3] // 2
    quarter = half // 2

    def up(i, by, n=4):
        return lax.rem(i + by, n)

    first_axis, second_axis = ("x", "y"), ("y", "x")
    a = (ix, iy)
    b = (iy, ix)
    step_of = (1, 3)
    group_by = (2, 1, 3, 0)

    def r1(h, k):
        return land.at[pl.ds((k * 2 + h) * 2, 2)]

    def d1(h, k):
        return land.at[pl.ds(16 + (k * 2 + h) * 4, 4)]

    def r2(h):
        return land.at[pl.ds(48 + h * 2, 2)]

    def d2(h):
        return land.at[pl.ds(52 + h * 4, 4)]

    def whole(ref, direction):
        return jnp.concatenate(
            [ref[direction * 2].astype(F32), ref[direction * 2 + 1].astype(F32)], axis=1
        )

    def cols(h, side=None):
        if side is None:
            return pl.ds(h * half, half)
        return pl.ds(h * half + side * quarter, quarter)

    def side_cols(side):
        return pl.ds(side * quarter, quarter)

    def block(h, ai, bi):
        return (bi, ai) if h == 0 else (ai, bi)

    def near(axis, i, direction):
        return {axis: up(i, step_of[direction])}

    def along_first(h, direction):
        return near(first_axis[h], a[h], direction)

    def along_second(h, direction):
        return near(second_axis[h], b[h], direction)

    def load(key, src, dst):
        pltpu.make_async_copy(src, dst, load_sems.at[LOADED[key]]).start()

    def loaded(key, dst):
        pltpu.make_async_copy(dst, dst, load_sems.at[LOADED[key]]).wait()

    for h in range(2):
        far = up(a[h], 2)
        src = g_hbm.at[:, far, :, cols(h)] if h == 0 else g_hbm.at[far, :, :, cols(h)]
        load(("gx",), src, gx.at[h])

    barrier = pltpu.get_barrier_semaphore()
    neighbours = [{"x": up(ix, s)} for s in step_of] + [{"y": up(iy, s)} for s in step_of]
    neighbours += [{"z": up(iz, s, z_size)} for s in (1, z_size - 1)]
    neighbours += [{"core": up(ic, s, n_core)} for s in range(1, n_core)]
    for device in neighbours:
        pl.semaphore_signal(barrier, inc=1, device_id=device, device_id_type=MESH)

    for h in range(2):
        load(("gv",), g_hbm.at[:, :, :, cols(h)], gv.at[h])
    for i, ref in enumerate((w_hbm, m_hbm, v_hbm)):
        load(("state",), ref, state.at[i])
    pl.semaphore_wait(barrier, len(neighbours))

    def tell(r):
        for s in (1, z_size - 1):
            pl.semaphore_signal(
                gossip.at[r], inc=1,
                device_id={"z": up(iz, s, z_size)}, device_id_type=MESH,
            )

    def told(r):
        pl.semaphore_wait(gossip.at[r], 2)

    def send(sent, key, src, dst, device):
        pltpu.make_async_remote_copy(
            src_ref=src,
            dst_ref=dst,
            send_sem=send_sems.at[SENT[sent,]],
            recv_sem=recv_sems.at[RECEIVED[key]],
            device_id=device,
            device_id_type=MESH,
        ).start()

    def arrived(key, bytes_of):
        pltpu.make_async_copy(bytes_of, bytes_of, recv_sems.at[RECEIVED[key]]).wait()

    def all_sent(sent, bytes_of):
        pltpu.make_async_copy(bytes_of, bytes_of, send_sems.at[SENT[sent,]]).wait()

    def send_far(k):
        for h in range(2):
            bi = up(b[h], group_by[k])
            for direction in range(2):
                send(
                    "rs", ("r1", k),
                    gx.at[h, bi, :, side_cols(direction)],
                    r1(h, k).at[direction],
                    along_first(h, direction),
                )

    def send_near(k):
        for h in range(2):
            bi = up(b[h], group_by[k])
            for direction in range(2):
                other = 1 - direction
                y, x = block(h, up(a[h], step_of[direction]), bi)
                send(
                    "rs", ("d1", k),
                    gv.at[h, y, x, :, side_cols(other)],
                    d1(h, k).at[direction * 2 + other],
                    along_first(h, direction),
                )

    def relay(k):
        arrived(("r1", k), land.at[pl.ds(k * 4, 4)])
        for h in range(2):
            bi = up(b[h], group_by[k])
            for direction in range(2):
                y, x = block(h, up(a[h], step_of[direction]), bi)
                x1[h, k, direction] = (
                    gv[h, y, x, :, side_cols(direction)].astype(F32)
                    + r1(h, k)[direction].astype(F32)
                ).astype(BF16)
                send(
                    "rs", ("d1", k),
                    x1.at[h, k, direction],
                    d1(h, k).at[direction * 2 + direction],
                    along_first(h, direction),
                )

    def complete(k):
        arrived(("d1", k), land.at[pl.ds(16 + k * 8, 8)])
        for h in range(2):
            bi = up(b[h], group_by[k])
            y, x = block(h, a[h], bi)
            total = gv[h, y, x].astype(F32) + whole(d1(h, k), 0) + whole(d1(h, k), 1)
            tf[h, k] = total
            if k < 3:
                tb[h, k] = total.astype(BF16)
            if k == 0:
                for direction in range(2):
                    send(
                        "rs", ("r2",),
                        tb.at[h, 0, :, side_cols(direction)],
                        r2(h).at[direction],
                        along_second(h, direction),
                    )
            if k in (1, 2):
                direction = k - 1
                other = 1 - direction
                send(
                    "rs", ("d2",),
                    tb.at[h, k, :, side_cols(other)],
                    d2(h).at[direction * 2 + other],
                    along_second(h, direction),
                )

    def relay_second():
        arrived(("r2",), land.at[pl.ds(48, 4)])
        for h in range(2):
            for direction in range(2):
                x2[h, direction] = (
                    tf[h, 1 + direction, :, side_cols(direction)]
                    + r2(h)[direction].astype(F32)
                ).astype(BF16)
                send(
                    "rs", ("d2",),
                    x2.at[h, direction],
                    d2(h).at[direction * 2 + direction],
                    along_second(h, direction),
                )

    loaded(("gx",), gx)
    for k in range(4):
        send_far(k)
    tell(0)
    loaded(("gv",), gv)
    send_near(0)
    relay(0)
    told(0)
    tell(1)
    send_near(1)
    relay(1)
    relay(2)
    told(1)
    tell(2)
    send_near(2)
    complete(0)
    relay(3)
    told(2)
    tell(3)
    complete(1)
    send_near(3)
    complete(2)
    relay_second()
    complete(3)
    told(3)
    loaded(("state",), state)

    lanes = jnp.zeros((8, 128), F32)
    arrived(("d2",), land.at[pl.ds(52, 8)])
    for h in range(2):
        total = tf[h, 3] + whole(d2(h), 0) + whole(d2(h), 1)
        tf[h, 3] = total
        square = total * total
        by_row = jnp.sum(square.reshape(-1, 8, half), axis=0)
        for c in range(half // 128):
            lanes = lanes + by_row[:, c * 128 : (c + 1) * 128]

    np_[0] = jnp.sum(lanes, axis=0, keepdims=True)
    distance = {0: 0, 1: 1, 2: 2, 3: 1}
    plane = sorted(
        ((i, j) for i in range(4) for j in range(4)),
        key=lambda at: -distance[at[0]] - distance[at[1]],
    )[:-1]
    for i, j in plane:
        slot = i * 4 + j
        send("np", ("np",), np_.at[0], np_.at[slot], {"y": up(iy, i), "x": up(ix, j)})
    arrived(("np",), np_.at[pl.ds(1, 15)])
    nz[0] = jnp.sum(np_[...], axis=0)
    line = sorted(
        ((i, j) for i in range(z_size) for j in range(n_core)),
        key=lambda at: -min(at[0], z_size - at[0]) - 0.5 * at[1],
    )[:-1]
    for i, j in line:
        slot = i * n_core + j
        device = {"z": up(iz, i, z_size), "core": up(ic, j, n_core)}
        send("nz", ("nz",), nz.at[0], nz.at[slot], device)
    arrived(("nz",), nz.at[pl.ds(1, len(line))])
    square_sum = jnp.sum(jnp.sum(nz[...], axis=0), axis=1, keepdims=True)
    limit = 0.5 * math.sqrt(entries)
    factor = jnp.minimum(1.0, limit / jnp.sqrt(square_sum + 1e-06))

    def update(h, side):
        at = cols(h, side)
        clipped = factor * tf[h, 3, :, side_cols(side)]
        new_first = 0.9 * state[1, :, at] + 0.1 * clipped
        new_second = 0.95 * state[2, :, at] + 0.05 * clipped * clipped
        first_hat = new_first * (1.0 / first_bias)
        second_hat = new_second * (1.0 / second_bias)
        master = state[0, :, at]
        new_master = master - 0.01 * (
            first_hat / (jnp.sqrt(second_hat) + 1e-08) + 0.1 * master
        )
        params[iy, ix, :, at] = new_master.astype(BF16)
        w_out[:, at] = new_master
        m_out[:, at] = new_first
        v_out[:, at] = new_second

    def piece(h, ai, bi, side):
        y, x = block(h, ai, bi)
        return params.at[y, x, :, cols(h, side)]

    arrived_from = (0, 3, 1, 2)

    two, four = x2.at[0], x2

    def gather_second(h, direction, side):
        part = piece(h, a[h], b[h], side)
        send("ag", ("g2", direction, side), part, part, along_second(h, direction))

    def forward_second(direction):
        arrived(("g2", direction, direction), two)
        for h in range(2):
            part = piece(h, a[h], up(b[h], step_of[1 - direction]), direction)
            send("ag", ("f2", direction), part, part, along_second(h, direction))

    def gather_first(j, side):
        if j in (1, 2) and side != j - 1:
            arrived(("g2", j - 1, side), two)
        if j == 3:
            arrived(("f2", side), two)
        for h in range(2):
            part = piece(h, a[h], up(b[h], arrived_from[j]), side)
            for direction in range(2):
                send("ag", ("g1", j, side), part, part, along_first(h, direction))

    def forward_first(j, direction):
        arrived(("g1", j, direction), four)
        for h in range(2):
            came_from = up(a[h], step_of[1 - direction])
            part = piece(h, came_from, up(b[h], arrived_from[j]), direction)
            send("ag", ("f1",), part, part, along_first(h, direction))

    for direction in range(2):
        for h in range(2):
            update(h, direction)
            gather_second(h, direction, direction)
    gather_first(0, 0)
    gather_first(0, 1)
    for h in range(2):
        for direction in range(2):
            gather_second(h, direction, 1 - direction)
    forward_second(0)
    gather_first(1, 0)
    forward_second(1)
    gather_first(2, 1)
    gather_first(1, 1)
    gather_first(3, 0)
    gather_first(2, 0)
    forward_first(1, 0)
    gather_first(3, 1)
    forward_first(0, 1)
    forward_first(0, 0)
    forward_first(1, 1)
    forward_first(2, 0)
    forward_first(2, 1)
    forward_first(3, 0)
    forward_first(3, 1)
    all_sent("rs", land)
    all_sent("np", np_.at[pl.ds(1, 15)])
    all_sent("nz", nz.at[pl.ds(1, len(line))])
    arrived(("f1",), x1)
    all_sent("ag", land)


def write_out(*refs):
    n = (len(refs) - 1) // 2
    sources, targets, sems = refs[:n], refs[n : 2 * n], refs[-1]
    copies = []
    for src, dst in zip(sources, targets):
        parts = [(src.at[i], dst.at[i]) for i in range(4)] if len(src.shape) == 4 else [(src, dst)]
        copies += parts
    made = [
        pltpu.make_async_copy(src, dst, sems.at[i]) for i, (src, dst) in enumerate(copies)
    ]
    for copy in made:
        copy.start()
    for copy in made:
        copy.wait()


def per_device(gradients, master_weights, first_moment, second_moment):
    rows, width = master_weights.shape
    entries = rows * lax.axis_size(DP) * lax.axis_size(SHARD) * width
    half, quarter = width // 2, width // 4
    grads = gradients.reshape(4, 4, rows, width)
    shapes = [((4, 4, rows, width), BF16)] + [((rows, width), F32)] * 3
    hbm = pl.BlockSpec(memory_space=pltpu.HBM)
    vmem = pl.BlockSpec(memory_space=pltpu.VMEM)
    z_size = lax.axis_size("z")
    results = pl.pallas_call(
        lambda *refs: kernel(entries, *refs),
        out_shape=[pltpu.VMEM(*shape) for shape in shapes],
        in_specs=[hbm] * 4,
        out_specs=[vmem] * 4,
        scratch_shapes=[
            pltpu.VMEM((2, 4, rows, half), BF16),
            pltpu.VMEM((2, 4, 4, rows, half), BF16),
            pltpu.VMEM((60, rows, quarter), BF16),
            pltpu.VMEM((2, 4, 2, rows, quarter), BF16),
            pltpu.VMEM((2, 4, rows, half), F32),
            pltpu.VMEM((2, 3, rows, half), BF16),
            pltpu.VMEM((2, 2, rows, quarter), BF16),
            pltpu.VMEM((3, rows, width), F32),
            pltpu.VMEM((16, 1, 128), F32),
            pltpu.VMEM((z_size * lax.axis_size("core"), 1, 128), F32),
            pltpu.SemaphoreType.DMA((len(LOADED),)),
            pltpu.SemaphoreType.DMA((len(SENT),)),
            pltpu.SemaphoreType.DMA((N_RECEIVED,)),
            pltpu.SemaphoreType.REGULAR((z_size // 2,)),
        ],
        compiler_params=pltpu.CompilerParams(
            collective_id=0, has_side_effects=True, vmem_limit_bytes=VMEM_LIMIT
        ),
    )(grads, master_weights, first_moment, second_moment)
    parameters, new_master, new_first, new_second = pl.pallas_call(
        write_out,
        out_shape=[jax.ShapeDtypeStruct(*shape) for shape in shapes],
        in_specs=[vmem] * 4,
        out_specs=[hbm] * 4,
        scratch_shapes=[pltpu.SemaphoreType.DMA((7,))],
        compiler_params=pltpu.CompilerParams(vmem_limit_bytes=2**20),
    )(*results)
    return (parameters.reshape(16 * rows, width), new_master, new_first, new_second)


def solution(mesh):
    split = Mesh(mesh.devices.reshape(4, 4, 8, 2), ("y", "x", "z", "core"))
    return jax.shard_map(
        per_device,
        mesh=split,
        in_specs=(P(DP, SHARD, None), P(SHARD_DP, None), P(SHARD_DP, None), P(SHARD_DP, None)),
        out_specs=(P(SHARD, None), P(SHARD_DP, None), P(SHARD_DP, None), P(SHARD_DP, None)),
        check_vma=False,
    )
```

```python
import math

import jax
import jax.numpy as jnp
from jax import lax
from jax.experimental import pallas as pl
from jax.experimental.pallas import tpu as pltpu
from jax.sharding import Mesh
from jax.sharding import PartitionSpec as P

DP = ("y", "x")
SHARD = ("z", "core")
SHARD_DP = ("z", "core", "y", "x")
MESH = pl.DeviceIdType.MESH

first_bias = 1.0 - math.exp(100.0 * math.log(0.9))
second_bias = 1.0 - math.exp(100.0 * math.log(0.95))

F32 = jnp.float32
BF16 = jnp.bfloat16
VMEM_LIMIT = 59 * 2**20


def table(*groups):
    keys = []
    for name, *dims in groups:
        index = [()]
        for dim in dims:
            index = [i + (j,) for i in index for j in range(dim)]
        keys += [(name, *i) for i in index]
    return {key: at for at, key in enumerate(keys)}


NORM = table(("norm",))
REDUCE = table(*NORM, ("r1", 4), ("d1", 4), ("r2",), ("d2",))
GATHER = table(*NORM, ("g2", 2, 2), ("f2", 2), ("g1", 4, 2), ("f1",))
RECEIVED = {**REDUCE, **GATHER}
N_RECEIVED = max(len(REDUCE), len(GATHER))
SENT = table(("rs",), ("norm",), ("ag",))
LOADED = table(("gx",), ("gv",), ("state",))


def kernel(
    entries,
    g_hbm, w_hbm, m_hbm, v_hbm,
    params, w_out, m_out, v_out,
    gx, gv, land, x1, tf, tb, x2, state, parts,
    load_sems, send_sems, recv_sems, gossip,
):
    ix, iy = lax.axis_index("x"), lax.axis_index("y")
    iz, ic = lax.axis_index("z"), lax.axis_index("core")
    z_size = lax.axis_size("z")
    n_core = lax.axis_size("core")
    half = g_hbm.shape[3] // 2
    quarter = half // 2

    def up(i, by, n=4):
        return lax.rem(i + by, n)

    first_axis, second_axis = ("x", "y"), ("y", "x")
    a = (ix, iy)
    b = (iy, ix)
    step_of = (1, 3)
    group_by = (2, 1, 3, 0)

    def r1(h, k):
        return land.at[pl.ds((k * 2 + h) * 2, 2)]

    def d1(h, k):
        return land.at[pl.ds(16 + (k * 2 + h) * 4, 4)]

    def r2(h):
        return land.at[pl.ds(48 + h * 2, 2)]

    def d2(h):
        return land.at[pl.ds(52 + h * 4, 4)]

    def whole(ref, direction):
        return jnp.concatenate(
            [ref[direction * 2].astype(F32), ref[direction * 2 + 1].astype(F32)], axis=1
        )

    def cols(h, side=None):
        if side is None:
            return pl.ds(h * half, half)
        return pl.ds(h * half + side * quarter, quarter)

    def side_cols(side):
        return pl.ds(side * quarter, quarter)

    def block(h, ai, bi):
        return (bi, ai) if h == 0 else (ai, bi)

    def near(axis, i, direction):
        return {axis: up(i, step_of[direction])}

    def along_first(h, direction):
        return near(first_axis[h], a[h], direction)

    def along_second(h, direction):
        return near(second_axis[h], b[h], direction)

    def load(key, src, dst):
        pltpu.make_async_copy(src, dst, load_sems.at[LOADED[key]]).start()

    def loaded(key, dst):
        pltpu.make_async_copy(dst, dst, load_sems.at[LOADED[key]]).wait()

    for h in range(2):
        far = up(a[h], 2)
        src = g_hbm.at[:, far, :, cols(h)] if h == 0 else g_hbm.at[far, :, :, cols(h)]
        load(("gx",), src, gx.at[h])

    barrier = pltpu.get_barrier_semaphore()
    neighbours = [{"x": up(ix, s)} for s in step_of] + [{"y": up(iy, s)} for s in step_of]
    neighbours += [{"z": up(iz, s, z_size)} for s in (1, z_size - 1)]
    neighbours += [{"core": up(ic, s, n_core)} for s in range(1, n_core)]
    for device in neighbours:
        pl.semaphore_signal(barrier, inc=1, device_id=device, device_id_type=MESH)

    for h in range(2):
        load(("gv",), g_hbm.at[:, :, :, cols(h)], gv.at[h])
    for i, ref in enumerate((w_hbm, m_hbm, v_hbm)):
        load(("state",), ref, state.at[i])
    pl.semaphore_wait(barrier, len(neighbours))

    links = {
        "x": [{"x": up(ix, s)} for s in step_of],
        "core": [{"core": up(ic, s, n_core)} for s in range(1, n_core)],
        "y": [{"y": up(iy, s)} for s in step_of],
        "z": [{"z": up(iz, s, z_size)} for s in (1, z_size - 1)],
    }
    rounds = ["x", "core", "y", "y"] + ["z"] * (z_size // 2)

    def tell(r):
        for device in links[rounds[r]]:
            pl.semaphore_signal(gossip.at[r], inc=1, device_id=device, device_id_type=MESH)

    def told(r):
        pl.semaphore_wait(gossip.at[r], len(links[rounds[r]]))

    def send(sent, key, src, dst, device):
        pltpu.make_async_remote_copy(
            src_ref=src,
            dst_ref=dst,
            send_sem=send_sems.at[SENT[sent,]],
            recv_sem=recv_sems.at[RECEIVED[key]],
            device_id=device,
            device_id_type=MESH,
        ).start()

    def arrived(key, bytes_of):
        pltpu.make_async_copy(bytes_of, bytes_of, recv_sems.at[RECEIVED[key]]).wait()

    def all_sent(sent, bytes_of):
        pltpu.make_async_copy(bytes_of, bytes_of, send_sems.at[SENT[sent,]]).wait()

    def send_far(k):
        for h in range(2):
            bi = up(b[h], group_by[k])
            for direction in range(2):
                send(
                    "rs", ("r1", k),
                    gx.at[h, bi, :, side_cols(direction)],
                    r1(h, k).at[direction],
                    along_first(h, direction),
                )

    def send_near(k):
        for h in range(2):
            bi = up(b[h], group_by[k])
            for direction in range(2):
                other = 1 - direction
                y, x = block(h, up(a[h], step_of[direction]), bi)
                send(
                    "rs", ("d1", k),
                    gv.at[h, y, x, :, side_cols(other)],
                    d1(h, k).at[direction * 2 + other],
                    along_first(h, direction),
                )

    def relay(k):
        arrived(("r1", k), land.at[pl.ds(k * 4, 4)])
        for h in range(2):
            bi = up(b[h], group_by[k])
            for direction in range(2):
                y, x = block(h, up(a[h], step_of[direction]), bi)
                x1[h, k, direction] = (
                    gv[h, y, x, :, side_cols(direction)].astype(F32)
                    + r1(h, k)[direction].astype(F32)
                ).astype(BF16)
                send(
                    "rs", ("d1", k),
                    x1.at[h, k, direction],
                    d1(h, k).at[direction * 2 + direction],
                    along_first(h, direction),
                )

    def complete(k):
        arrived(("d1", k), land.at[pl.ds(16 + k * 8, 8)])
        for h in range(2):
            bi = up(b[h], group_by[k])
            y, x = block(h, a[h], bi)
            total = gv[h, y, x].astype(F32) + whole(d1(h, k), 0) + whole(d1(h, k), 1)
            tf[h, k] = total
            if k < 3:
                tb[h, k] = total.astype(BF16)
            if k == 0:
                for direction in range(2):
                    send(
                        "rs", ("r2",),
                        tb.at[h, 0, :, side_cols(direction)],
                        r2(h).at[direction],
                        along_second(h, direction),
                    )
            if k in (1, 2):
                direction = k - 1
                other = 1 - direction
                send(
                    "rs", ("d2",),
                    tb.at[h, k, :, side_cols(other)],
                    d2(h).at[direction * 2 + other],
                    along_second(h, direction),
                )

    def relay_second():
        arrived(("r2",), land.at[pl.ds(48, 4)])
        for h in range(2):
            for direction in range(2):
                x2[h, direction] = (
                    tf[h, 1 + direction, :, side_cols(direction)]
                    + r2(h)[direction].astype(F32)
                ).astype(BF16)
                send(
                    "rs", ("d2",),
                    x2.at[h, direction],
                    d2(h).at[direction * 2 + direction],
                    along_second(h, direction),
                )

    loaded(("gx",), gx)
    for k in range(4):
        send_far(k)
    tell(0)
    loaded(("gv",), gv)
    send_near(0)
    told(0)
    tell(1)
    told(1)
    tell(2)
    told(2)
    tell(3)
    relay(0)
    send_near(1)
    told(3)
    tell(4)
    relay(1)
    relay(2)
    told(4)
    tell(5)
    send_near(2)
    complete(0)
    told(5)
    tell(6)
    relay(3)
    complete(1)
    told(6)
    tell(7)
    send_near(3)
    complete(2)
    relay_second()
    complete(3)
    for r in range(7, len(rounds)):
        told(r)
        if r + 1 < len(rounds):
            tell(r + 1)
    loaded(("state",), state)

    lanes = jnp.zeros((8, 128), F32)
    arrived(("d2",), land.at[pl.ds(52, 8)])
    for h in range(2):
        total = tf[h, 3] + whole(d2(h), 0) + whole(d2(h), 1)
        tf[h, 3] = total
        square = total * total
        by_row = jnp.sum(square.reshape(-1, 8, half), axis=0)
        for c in range(half // 128):
            lanes = lanes + by_row[:, c * 128 : (c + 1) * 128]

    me = ((iz * n_core + ic) * 4 + iy) * 4 + ix
    parts[me] = jnp.sum(lanes, axis=0, keepdims=True)

    def tell_part(device):
        send("norm", ("norm",), parts.at[me], parts.at[me], device)

    def tell_row(z, i):
        for x in range(4):
            tell_part({"z": z, "core": i // 4, "y": lax.rem(i, 4), "x": x})

    for z in (0, 1, 2, 3, 7, 4, 5, 6):
        @pl.when(z != iz)
        def _():
            lax.fori_loop(0, 4 * n_core, lambda i, c: (tell_row(z, i), c)[1], 0)

    for i in range(n_core):
        for y in range(4):
            for x in range(4):
                if (i, y, x) != (0, 0, 0):
                    tell_part({"core": up(ic, i, n_core), "y": up(iy, y), "x": up(ix, x)})

    n_all = 16 * z_size * n_core
    arrived(("norm",), parts.at[pl.ds(0, n_all - 1)])
    square_sum = jnp.sum(jnp.sum(parts[...], axis=0), axis=1, keepdims=True)
    limit = 0.5 * math.sqrt(entries)
    factor = jnp.minimum(1.0, limit / jnp.sqrt(square_sum + 1e-06))

    def update(h, side):
        at = cols(h, side)
        clipped = factor * tf[h, 3, :, side_cols(side)]
        new_first = 0.9 * state[1, :, at] + 0.1 * clipped
        new_second = 0.95 * state[2, :, at] + 0.05 * clipped * clipped
        first_hat = new_first * (1.0 / first_bias)
        second_hat = new_second * (1.0 / second_bias)
        master = state[0, :, at]
        new_master = master - 0.01 * (
            first_hat / (jnp.sqrt(second_hat) + 1e-08) + 0.1 * master
        )
        params[iy, ix, :, at] = new_master.astype(BF16)
        w_out[:, at] = new_master
        m_out[:, at] = new_first
        v_out[:, at] = new_second

    def piece(h, ai, bi, side):
        y, x = block(h, ai, bi)
        return params.at[y, x, :, cols(h, side)]

    arrived_from = (0, 3, 1, 2)

    two, four = x2.at[0], x2

    def gather_second(h, direction, side):
        part = piece(h, a[h], b[h], side)
        send("ag", ("g2", direction, side), part, part, along_second(h, direction))

    def forward_second(direction):
        arrived(("g2", direction, direction), two)
        for h in range(2):
            part = piece(h, a[h], up(b[h], step_of[1 - direction]), direction)
            send("ag", ("f2", direction), part, part, along_second(h, direction))

    def gather_first(j, side):
        if j in (1, 2) and side != j - 1:
            arrived(("g2", j - 1, side), two)
        if j == 3:
            arrived(("f2", side), two)
        for h in range(2):
            part = piece(h, a[h], up(b[h], arrived_from[j]), side)
            for direction in range(2):
                send("ag", ("g1", j, side), part, part, along_first(h, direction))

    def forward_first(j, direction):
        arrived(("g1", j, direction), four)
        for h in range(2):
            came_from = up(a[h], step_of[1 - direction])
            part = piece(h, came_from, up(b[h], arrived_from[j]), direction)
            send("ag", ("f1",), part, part, along_first(h, direction))

    for direction in range(2):
        for h in range(2):
            update(h, direction)
            gather_second(h, direction, direction)
    gather_first(0, 0)
    gather_first(0, 1)
    for h in range(2):
        for direction in range(2):
            gather_second(h, direction, 1 - direction)
    forward_second(0)
    gather_first(1, 0)
    forward_second(1)
    gather_first(2, 1)
    gather_first(1, 1)
    gather_first(3, 0)
    gather_first(2, 0)
    forward_first(1, 0)
    gather_first(3, 1)
    forward_first(0, 1)
    forward_first(0, 0)
    forward_first(1, 1)
    forward_first(2, 0)
    forward_first(2, 1)
    forward_first(3, 0)
    forward_first(3, 1)
    all_sent("rs", land)
    all_sent("norm", parts.at[pl.ds(0, n_all - 1)])
    arrived(("f1",), x1)
    all_sent("ag", land)


def write_out(*refs):
    n = (len(refs) - 1) // 2
    sources, targets, sems = refs[:n], refs[n : 2 * n], refs[-1]
    copies = []
    for src, dst in zip(sources, targets):
        parts = [(src.at[i], dst.at[i]) for i in range(4)] if len(src.shape) == 4 else [(src, dst)]
        copies += parts
    made = [
        pltpu.make_async_copy(src, dst, sems.at[i]) for i, (src, dst) in enumerate(copies)
    ]
    for copy in made:
        copy.start()
    for copy in made:
        copy.wait()


def per_device(gradients, master_weights, first_moment, second_moment):
    rows, width = master_weights.shape
    entries = rows * lax.axis_size(DP) * lax.axis_size(SHARD) * width
    half, quarter = width // 2, width // 4
    grads = gradients.reshape(4, 4, rows, width)
    shapes = [((4, 4, rows, width), BF16)] + [((rows, width), F32)] * 3
    hbm = pl.BlockSpec(memory_space=pltpu.HBM)
    vmem = pl.BlockSpec(memory_space=pltpu.VMEM)
    z_size = lax.axis_size("z")
    results = pl.pallas_call(
        lambda *refs: kernel(entries, *refs),
        out_shape=[pltpu.VMEM(*shape) for shape in shapes],
        in_specs=[hbm] * 4,
        out_specs=[vmem] * 4,
        scratch_shapes=[
            pltpu.VMEM((2, 4, rows, half), BF16),
            pltpu.VMEM((2, 4, 4, rows, half), BF16),
            pltpu.VMEM((60, rows, quarter), BF16),
            pltpu.VMEM((2, 4, 2, rows, quarter), BF16),
            pltpu.VMEM((2, 4, rows, half), F32),
            pltpu.VMEM((2, 3, rows, half), BF16),
            pltpu.VMEM((2, 2, rows, quarter), BF16),
            pltpu.VMEM((3, rows, width), F32),
            pltpu.VMEM((16 * z_size * lax.axis_size("core"), 1, 128), F32),
            pltpu.SemaphoreType.DMA((len(LOADED),)),
            pltpu.SemaphoreType.DMA((len(SENT),)),
            pltpu.SemaphoreType.DMA((N_RECEIVED,)),
            pltpu.SemaphoreType.REGULAR((4 + z_size // 2,)),
        ],
        compiler_params=pltpu.CompilerParams(
            collective_id=0, has_side_effects=True, vmem_limit_bytes=VMEM_LIMIT
        ),
    )(grads, master_weights, first_moment, second_moment)
    parameters, new_master, new_first, new_second = pl.pallas_call(
        write_out,
        out_shape=[jax.ShapeDtypeStruct(*shape) for shape in shapes],
        in_specs=[vmem] * 4,
        out_specs=[hbm] * 4,
        scratch_shapes=[pltpu.SemaphoreType.DMA((7,))],
        compiler_params=pltpu.CompilerParams(vmem_limit_bytes=2**20),
    )(*results)
    return (parameters.reshape(16 * rows, width), new_master, new_first, new_second)


def solution(mesh):
    split = Mesh(mesh.devices.reshape(4, 4, 8, 2), ("y", "x", "z", "core"))
    return jax.shard_map(
        per_device,
        mesh=split,
        in_specs=(P(DP, SHARD, None), P(SHARD_DP, None), P(SHARD_DP, None), P(SHARD_DP, None)),
        out_specs=(P(SHARD, None), P(SHARD_DP, None), P(SHARD_DP, None), P(SHARD_DP, None)),
        check_vma=False,
    )
```

```python
import math

import jax
import jax.numpy as jnp
from jax import lax
from jax.experimental import pallas as pl
from jax.experimental.pallas import tpu as pltpu
from jax.sharding import Mesh
from jax.sharding import PartitionSpec as P

DP = ("y", "x")
SHARD = ("z", "core")
SHARD_DP = ("z", "core", "y", "x")
MESH = pl.DeviceIdType.MESH

first_bias = 1.0 - math.exp(100.0 * math.log(0.9))
second_bias = 1.0 - math.exp(100.0 * math.log(0.95))

F32 = jnp.float32
BF16 = jnp.bfloat16
VMEM_LIMIT = 59 * 2**20


def table(*groups):
    keys = []
    for name, *dims in groups:
        index = [()]
        for dim in dims:
            index = [i + (j,) for i in index for j in range(dim)]
        keys += [(name, *i) for i in index]
    return {key: at for at, key in enumerate(keys)}


NORM = table(("norm",))
REDUCE = table(*NORM, ("r1", 4), ("d1", 4), ("r2",), ("d2",))
GATHER = table(*NORM, ("g2", 2, 2), ("f2", 2), ("g1", 4, 2), ("f1",))
RECEIVED = {**REDUCE, **GATHER}
N_RECEIVED = max(len(REDUCE), len(GATHER))
SENT = table(("rs",), ("norm",), ("ag",))
LOADED = table(("gx",), ("gv",), ("state",))


def kernel(
    entries,
    g_hbm, w_hbm, m_hbm, v_hbm,
    params, w_out, m_out, v_out,
    gx, gv, land, x1, tf, tb, x2, state, parts,
    load_sems, send_sems, recv_sems, gossip,
):
    ix, iy = lax.axis_index("x"), lax.axis_index("y")
    iz, ic = lax.axis_index("z"), lax.axis_index("core")
    z_size = lax.axis_size("z")
    n_core = lax.axis_size("core")
    half = g_hbm.shape[3] // 2
    quarter = half // 2

    def up(i, by, n=4):
        return lax.rem(i + by, n)

    first_axis, second_axis = ("x", "y"), ("y", "x")
    a = (ix, iy)
    b = (iy, ix)
    step_of = (1, 3)
    group_by = (2, 1, 3, 0)

    def r1(h, k):
        return land.at[pl.ds((k * 2 + h) * 2, 2)]

    def d1(h, k):
        return land.at[pl.ds(16 + (k * 2 + h) * 4, 4)]

    def r2(h):
        return land.at[pl.ds(48 + h * 2, 2)]

    def d2(h):
        return land.at[pl.ds(52 + h * 4, 4)]

    def whole(ref, direction):
        return jnp.concatenate(
            [ref[direction * 2].astype(F32), ref[direction * 2 + 1].astype(F32)], axis=1
        )

    def cols(h, side=None):
        if side is None:
            return pl.ds(h * half, half)
        return pl.ds(h * half + side * quarter, quarter)

    def side_cols(side):
        return pl.ds(side * quarter, quarter)

    def block(h, ai, bi):
        return (bi, ai) if h == 0 else (ai, bi)

    def near(axis, i, direction):
        return {axis: up(i, step_of[direction])}

    def along_first(h, direction):
        return near(first_axis[h], a[h], direction)

    def along_second(h, direction):
        return near(second_axis[h], b[h], direction)

    def load(key, src, dst):
        pltpu.make_async_copy(src, dst, load_sems.at[LOADED[key]]).start()

    def loaded(key, dst):
        pltpu.make_async_copy(dst, dst, load_sems.at[LOADED[key]]).wait()

    barrier = pltpu.get_barrier_semaphore()
    neighbours = [{"x": up(ix, s)} for s in step_of] + [{"y": up(iy, s)} for s in step_of]
    neighbours += [{"z": up(iz, s, z_size)} for s in (1, z_size - 1)]
    neighbours += [{"core": up(ic, s, n_core)} for s in range(1, n_core)]
    for device in neighbours:
        pl.semaphore_signal(barrier, inc=1, device_id=device, device_id_type=MESH)

    for h in range(2):
        far = up(a[h], 2)
        src = g_hbm.at[:, far, :, cols(h)] if h == 0 else g_hbm.at[far, :, :, cols(h)]
        load(("gx",), src, gx.at[h])
    for h in range(2):
        load(("gv",), g_hbm.at[:, :, :, cols(h)], gv.at[h])
    for i, ref in enumerate((w_hbm, m_hbm, v_hbm)):
        load(("state",), ref, state.at[i])
    pl.semaphore_wait(barrier, len(neighbours))

    links = {
        "x": [{"x": up(ix, s)} for s in step_of],
        "core": [{"core": up(ic, s, n_core)} for s in range(1, n_core)],
        "y": [{"y": up(iy, s)} for s in step_of],
        "z": [{"z": up(iz, s, z_size)} for s in (1, z_size - 1)],
    }
    rounds = ["x", "core", "y", "y"] + ["z"] * (z_size // 2)

    def tell(r):
        for device in links[rounds[r]]:
            pl.semaphore_signal(gossip.at[r], inc=1, device_id=device, device_id_type=MESH)

    def told(r):
        pl.semaphore_wait(gossip.at[r], len(links[rounds[r]]))

    def send(sent, key, src, dst, device):
        pltpu.make_async_remote_copy(
            src_ref=src,
            dst_ref=dst,
            send_sem=send_sems.at[SENT[sent,]],
            recv_sem=recv_sems.at[RECEIVED[key]],
            device_id=device,
            device_id_type=MESH,
        ).start()

    def arrived(key, bytes_of):
        pltpu.make_async_copy(bytes_of, bytes_of, recv_sems.at[RECEIVED[key]]).wait()

    def all_sent(sent, bytes_of):
        pltpu.make_async_copy(bytes_of, bytes_of, send_sems.at[SENT[sent,]]).wait()

    def send_far(k):
        for h in range(2):
            bi = up(b[h], group_by[k])
            for direction in range(2):
                send(
                    "rs", ("r1", k),
                    gx.at[h, bi, :, side_cols(direction)],
                    r1(h, k).at[direction],
                    along_first(h, direction),
                )

    def send_near(k):
        for h in range(2):
            bi = up(b[h], group_by[k])
            for direction in range(2):
                other = 1 - direction
                y, x = block(h, up(a[h], step_of[direction]), bi)
                send(
                    "rs", ("d1", k),
                    gv.at[h, y, x, :, side_cols(other)],
                    d1(h, k).at[direction * 2 + other],
                    along_first(h, direction),
                )

    def relay(k):
        arrived(("r1", k), land.at[pl.ds(k * 4, 4)])
        for h in range(2):
            bi = up(b[h], group_by[k])
            for direction in range(2):
                y, x = block(h, up(a[h], step_of[direction]), bi)
                x1[h, k, direction] = (
                    gv[h, y, x, :, side_cols(direction)].astype(F32)
                    + r1(h, k)[direction].astype(F32)
                ).astype(BF16)
                send(
                    "rs", ("d1", k),
                    x1.at[h, k, direction],
                    d1(h, k).at[direction * 2 + direction],
                    along_first(h, direction),
                )

    def complete(k):
        arrived(("d1", k), land.at[pl.ds(16 + k * 8, 8)])
        for h in range(2):
            bi = up(b[h], group_by[k])
            y, x = block(h, a[h], bi)
            total = gv[h, y, x].astype(F32) + whole(d1(h, k), 0) + whole(d1(h, k), 1)
            tf[h, k] = total
            if k < 3:
                tb[h, k] = total.astype(BF16)
            if k == 0:
                for direction in range(2):
                    send(
                        "rs", ("r2",),
                        tb.at[h, 0, :, side_cols(direction)],
                        r2(h).at[direction],
                        along_second(h, direction),
                    )
            if k in (1, 2):
                direction = k - 1
                other = 1 - direction
                send(
                    "rs", ("d2",),
                    tb.at[h, k, :, side_cols(other)],
                    d2(h).at[direction * 2 + other],
                    along_second(h, direction),
                )

    def relay_second():
        arrived(("r2",), land.at[pl.ds(48, 4)])
        for h in range(2):
            for direction in range(2):
                x2[h, direction] = (
                    tf[h, 1 + direction, :, side_cols(direction)]
                    + r2(h)[direction].astype(F32)
                ).astype(BF16)
                send(
                    "rs", ("d2",),
                    x2.at[h, direction],
                    d2(h).at[direction * 2 + direction],
                    along_second(h, direction),
                )

    loaded(("gx",), gx)
    for k in range(4):
        send_far(k)
    tell(0)
    loaded(("gv",), gv)
    send_near(0)
    told(0)
    tell(1)
    told(1)
    tell(2)
    told(2)
    tell(3)
    relay(0)
    send_near(1)
    told(3)
    tell(4)
    relay(1)
    relay(2)
    told(4)
    tell(5)
    send_near(2)
    complete(0)
    told(5)
    tell(6)
    relay(3)
    complete(1)
    told(6)
    tell(7)
    send_near(3)
    complete(2)
    relay_second()
    complete(3)
    for r in range(7, len(rounds)):
        told(r)
        if r + 1 < len(rounds):
            tell(r + 1)
    loaded(("state",), state)

    lanes = jnp.zeros((8, 128), F32)
    arrived(("d2",), land.at[pl.ds(52, 8)])
    for h in range(2):
        total = tf[h, 3] + whole(d2(h), 0) + whole(d2(h), 1)
        tf[h, 3] = total
        square = total * total
        by_row = jnp.sum(square.reshape(-1, 8, half), axis=0)
        for c in range(half // 128):
            lanes = lanes + by_row[:, c * 128 : (c + 1) * 128]

    me = ((iz * n_core + ic) * 4 + iy) * 4 + ix
    parts[me] = jnp.sum(lanes, axis=0, keepdims=True)

    def tell_part(device):
        send("norm", ("norm",), parts.at[me], parts.at[me], device)

    def tell_row(z, i):
        for x in range(4):
            tell_part({"z": z, "core": i // 4, "y": lax.rem(i, 4), "x": x})

    for z in (0, 1, 2, 3, 7, 4, 5, 6):
        @pl.when(z != iz)
        def _():
            lax.fori_loop(0, 4 * n_core, lambda i, c: (tell_row(z, i), c)[1], 0)

    for i in range(n_core):
        for y in range(4):
            for x in range(4):
                if (i, y, x) != (0, 0, 0):
                    tell_part({"core": up(ic, i, n_core), "y": up(iy, y), "x": up(ix, x)})

    n_all = 16 * z_size * n_core
    arrived(("norm",), parts.at[pl.ds(0, n_all - 1)])
    rest = [parts[i] for i in range(n_all)]
    while len(rest) > 1:
        rest = [p + q for p, q in zip(rest[::2], rest[1::2])]
    square_sum = jnp.sum(rest[0], axis=1, keepdims=True)
    limit = 0.5 * math.sqrt(entries)
    factor = jnp.minimum(1.0, limit / jnp.sqrt(square_sum + 1e-06))

    def update(h, side):
        at = cols(h, side)
        clipped = factor * tf[h, 3, :, side_cols(side)]
        new_first = 0.9 * state[1, :, at] + 0.1 * clipped
        new_second = 0.95 * state[2, :, at] + 0.05 * clipped * clipped
        first_hat = new_first * (1.0 / first_bias)
        second_hat = new_second * (1.0 / second_bias)
        master = state[0, :, at]
        new_master = master - 0.01 * (
            first_hat / (jnp.sqrt(second_hat) + 1e-08) + 0.1 * master
        )
        params[iy, ix, :, at] = new_master.astype(BF16)
        w_out[:, at] = new_master
        m_out[:, at] = new_first
        v_out[:, at] = new_second

    def piece(h, ai, bi, side):
        y, x = block(h, ai, bi)
        return params.at[y, x, :, cols(h, side)]

    arrived_from = (0, 3, 1, 2)

    two, four = x2.at[0], x2

    def gather_second(h, direction, side):
        part = piece(h, a[h], b[h], side)
        send("ag", ("g2", direction, side), part, part, along_second(h, direction))

    def forward_second(direction):
        arrived(("g2", direction, direction), two)
        for h in range(2):
            part = piece(h, a[h], up(b[h], step_of[1 - direction]), direction)
            send("ag", ("f2", direction), part, part, along_second(h, direction))

    def gather_first(j, side):
        if j in (1, 2) and side != j - 1:
            arrived(("g2", j - 1, side), two)
        if j == 3:
            arrived(("f2", side), two)
        for h in range(2):
            part = piece(h, a[h], up(b[h], arrived_from[j]), side)
            for direction in range(2):
                send("ag", ("g1", j, side), part, part, along_first(h, direction))

    def forward_first(j, direction):
        arrived(("g1", j, direction), four)
        for h in range(2):
            came_from = up(a[h], step_of[1 - direction])
            part = piece(h, came_from, up(b[h], arrived_from[j]), direction)
            send("ag", ("f1",), part, part, along_first(h, direction))

    for direction in range(2):
        for h in range(2):
            update(h, direction)
            gather_second(h, direction, direction)
    gather_first(0, 0)
    gather_first(0, 1)
    for h in range(2):
        for direction in range(2):
            gather_second(h, direction, 1 - direction)
    forward_second(0)
    gather_first(1, 0)
    forward_second(1)
    gather_first(2, 1)
    gather_first(1, 1)
    gather_first(3, 0)
    gather_first(2, 0)
    forward_first(1, 0)
    gather_first(3, 1)
    forward_first(0, 1)
    forward_first(0, 0)
    forward_first(1, 1)
    forward_first(2, 0)
    forward_first(2, 1)
    forward_first(3, 0)
    forward_first(3, 1)
    all_sent("rs", land)
    all_sent("norm", parts.at[pl.ds(0, n_all - 1)])
    arrived(("f1",), x1)
    all_sent("ag", land)


def write_out(*refs):
    n = (len(refs) - 1) // 2
    sources, targets, sems = refs[:n], refs[n : 2 * n], refs[-1]
    copies = []
    for src, dst in zip(sources, targets):
        parts = [(src.at[i], dst.at[i]) for i in range(4)] if len(src.shape) == 4 else [(src, dst)]
        copies += parts
    made = [
        pltpu.make_async_copy(src, dst, sems.at[i]) for i, (src, dst) in enumerate(copies)
    ]
    for copy in made:
        copy.start()
    for copy in made:
        copy.wait()


def per_device(gradients, master_weights, first_moment, second_moment):
    rows, width = master_weights.shape
    entries = rows * lax.axis_size(DP) * lax.axis_size(SHARD) * width
    half, quarter = width // 2, width // 4
    grads = gradients.reshape(4, 4, rows, width)
    shapes = [((4, 4, rows, width), BF16)] + [((rows, width), F32)] * 3
    hbm = pl.BlockSpec(memory_space=pltpu.HBM)
    vmem = pl.BlockSpec(memory_space=pltpu.VMEM)
    z_size = lax.axis_size("z")
    results = pl.pallas_call(
        lambda *refs: kernel(entries, *refs),
        out_shape=[pltpu.VMEM(*shape) for shape in shapes],
        in_specs=[hbm] * 4,
        out_specs=[vmem] * 4,
        scratch_shapes=[
            pltpu.VMEM((2, 4, rows, half), BF16),
            pltpu.VMEM((2, 4, 4, rows, half), BF16),
            pltpu.VMEM((60, rows, quarter), BF16),
            pltpu.VMEM((2, 4, 2, rows, quarter), BF16),
            pltpu.VMEM((2, 4, rows, half), F32),
            pltpu.VMEM((2, 3, rows, half), BF16),
            pltpu.VMEM((2, 2, rows, quarter), BF16),
            pltpu.VMEM((3, rows, width), F32),
            pltpu.VMEM((16 * z_size * lax.axis_size("core"), 1, 128), F32),
            pltpu.SemaphoreType.DMA((len(LOADED),)),
            pltpu.SemaphoreType.DMA((len(SENT),)),
            pltpu.SemaphoreType.DMA((N_RECEIVED,)),
            pltpu.SemaphoreType.REGULAR((4 + z_size // 2,)),
        ],
        compiler_params=pltpu.CompilerParams(
            collective_id=0, has_side_effects=True, vmem_limit_bytes=VMEM_LIMIT
        ),
    )(grads, master_weights, first_moment, second_moment)
    parameters, new_master, new_first, new_second = pl.pallas_call(
        write_out,
        out_shape=[jax.ShapeDtypeStruct(*shape) for shape in shapes],
        in_specs=[vmem] * 4,
        out_specs=[hbm] * 4,
        scratch_shapes=[pltpu.SemaphoreType.DMA((7,))],
        compiler_params=pltpu.CompilerParams(vmem_limit_bytes=2**20),
    )(*results)
    return (parameters.reshape(16 * rows, width), new_master, new_first, new_second)


def solution(mesh):
    split = Mesh(mesh.devices.reshape(4, 4, 8, 2), ("y", "x", "z", "core"))
    return jax.shard_map(
        per_device,
        mesh=split,
        in_specs=(P(DP, SHARD, None), P(SHARD_DP, None), P(SHARD_DP, None), P(SHARD_DP, None)),
        out_specs=(P(SHARD, None), P(SHARD_DP, None), P(SHARD_DP, None), P(SHARD_DP, None)),
        check_vma=False,
    )
```

```python
import math

import jax
import jax.numpy as jnp
from jax import lax
from jax.experimental import pallas as pl
from jax.experimental.pallas import tpu as pltpu
from jax.sharding import Mesh
from jax.sharding import PartitionSpec as P

DP = ("y", "x")
SHARD = ("z", "core")
SHARD_DP = ("z", "core", "y", "x")
MESH = pl.DeviceIdType.MESH

first_bias = 1.0 - math.exp(100.0 * math.log(0.9))
second_bias = 1.0 - math.exp(100.0 * math.log(0.95))

F32 = jnp.float32
BF16 = jnp.bfloat16
VMEM_LIMIT = 59 * 2**20


def table(*groups):
    keys = []
    for name, *dims in groups:
        index = [()]
        for dim in dims:
            index = [i + (j,) for i in index for j in range(dim)]
        keys += [(name, *i) for i in index]
    return {key: at for at, key in enumerate(keys)}


NORM = table(("norm",))
REDUCE = table(*NORM, ("r1", 4), ("d1", 4), ("r2",), ("d2",))
GATHER = table(*NORM, ("g2", 2, 2), ("f2", 2), ("g1", 4, 2), ("f1",))
RECEIVED = {**REDUCE, **GATHER}
N_RECEIVED = max(len(REDUCE), len(GATHER))
SENT = table(("rs",), ("norm",), ("ag",))
LOADED = table(("gx",), ("gv",), ("state",))


def kernel(
    entries,
    g_hbm, w_hbm, m_hbm, v_hbm,
    params, w_out, m_out, v_out,
    gx, gv, land, x1, tf, tb, x2, state, parts,
    load_sems, send_sems, recv_sems, gossip,
):
    ix, iy = lax.axis_index("x"), lax.axis_index("y")
    iz, ic = lax.axis_index("z"), lax.axis_index("core")
    z_size = lax.axis_size("z")
    n_core = lax.axis_size("core")
    half = g_hbm.shape[3] // 2
    quarter = half // 2

    def up(i, by, n=4):
        return lax.rem(i + by, n)

    first_axis, second_axis = ("x", "y"), ("y", "x")
    a = (ix, iy)
    b = (iy, ix)
    step_of = (1, 3)
    group_by = (2, 1, 3, 0)

    def r1(h, k):
        return land.at[pl.ds((k * 2 + h) * 2, 2)]

    def d1(h, k):
        return land.at[pl.ds(16 + (k * 2 + h) * 4, 4)]

    def r2(h):
        return land.at[pl.ds(48 + h * 2, 2)]

    def d2(h):
        return land.at[pl.ds(52 + h * 4, 4)]

    def whole(ref, direction):
        return jnp.concatenate(
            [ref[direction * 2].astype(F32), ref[direction * 2 + 1].astype(F32)], axis=1
        )

    def cols(h, side=None):
        if side is None:
            return pl.ds(h * half, half)
        return pl.ds(h * half + side * quarter, quarter)

    def side_cols(side):
        return pl.ds(side * quarter, quarter)

    def block(h, ai, bi):
        return (bi, ai) if h == 0 else (ai, bi)

    def near(axis, i, direction):
        return {axis: up(i, step_of[direction])}

    def along_first(h, direction):
        return near(first_axis[h], a[h], direction)

    def along_second(h, direction):
        return near(second_axis[h], b[h], direction)

    def load(key, src, dst):
        pltpu.make_async_copy(src, dst, load_sems.at[LOADED[key]]).start()

    def loaded(key, dst):
        pltpu.make_async_copy(dst, dst, load_sems.at[LOADED[key]]).wait()

    barrier = pltpu.get_barrier_semaphore()
    neighbours = [{"x": up(ix, s)} for s in step_of] + [{"y": up(iy, s)} for s in step_of]
    neighbours += [{"z": up(iz, s, z_size)} for s in (1, z_size - 1)]
    neighbours += [{"core": up(ic, s, n_core)} for s in range(1, n_core)]
    for device in neighbours:
        pl.semaphore_signal(barrier, inc=1, device_id=device, device_id_type=MESH)

    for h in range(2):
        far = up(a[h], 2)
        src = g_hbm.at[:, far, :, cols(h)] if h == 0 else g_hbm.at[far, :, :, cols(h)]
        load(("gx",), src, gx.at[h])
    for h in range(2):
        load(("gv",), g_hbm.at[:, :, :, cols(h)], gv.at[h])
    for i, ref in enumerate((w_hbm, m_hbm, v_hbm)):
        load(("state",), ref, state.at[i])
    pl.semaphore_wait(barrier, len(neighbours))

    links = {
        "x": [{"x": up(ix, s)} for s in step_of],
        "core": [{"core": up(ic, s, n_core)} for s in range(1, n_core)],
        "y": [{"y": up(iy, s)} for s in step_of],
        "z": [{"z": up(iz, s, z_size)} for s in (1, z_size - 1)],
    }
    rounds = ["x", "core", "y", "y"] + ["z"] * (z_size // 2)

    def tell(r):
        for device in links[rounds[r]]:
            pl.semaphore_signal(gossip.at[r], inc=1, device_id=device, device_id_type=MESH)

    def told(r):
        pl.semaphore_wait(gossip.at[r], len(links[rounds[r]]))

    def send(sent, key, src, dst, device):
        pltpu.make_async_remote_copy(
            src_ref=src,
            dst_ref=dst,
            send_sem=send_sems.at[SENT[sent,]],
            recv_sem=recv_sems.at[RECEIVED[key]],
            device_id=device,
            device_id_type=MESH,
        ).start()

    def arrived(key, bytes_of):
        pltpu.make_async_copy(bytes_of, bytes_of, recv_sems.at[RECEIVED[key]]).wait()

    def all_sent(sent, bytes_of):
        pltpu.make_async_copy(bytes_of, bytes_of, send_sems.at[SENT[sent,]]).wait()

    def send_far(k):
        for h in range(2):
            bi = up(b[h], group_by[k])
            for direction in range(2):
                send(
                    "rs", ("r1", k),
                    gx.at[h, bi, :, side_cols(direction)],
                    r1(h, k).at[direction],
                    along_first(h, direction),
                )

    def send_near(k):
        for h in range(2):
            bi = up(b[h], group_by[k])
            for direction in range(2):
                other = 1 - direction
                y, x = block(h, up(a[h], step_of[direction]), bi)
                send(
                    "rs", ("d1", k),
                    gv.at[h, y, x, :, side_cols(other)],
                    d1(h, k).at[direction * 2 + other],
                    along_first(h, direction),
                )

    def relay(k):
        arrived(("r1", k), land.at[pl.ds(k * 4, 4)])
        for h in range(2):
            bi = up(b[h], group_by[k])
            for direction in range(2):
                y, x = block(h, up(a[h], step_of[direction]), bi)
                x1[h, k, direction] = (
                    gv[h, y, x, :, side_cols(direction)].astype(F32)
                    + r1(h, k)[direction].astype(F32)
                ).astype(BF16)
                send(
                    "rs", ("d1", k),
                    x1.at[h, k, direction],
                    d1(h, k).at[direction * 2 + direction],
                    along_first(h, direction),
                )

    def complete(k):
        arrived(("d1", k), land.at[pl.ds(16 + k * 8, 8)])
        for h in range(2):
            bi = up(b[h], group_by[k])
            y, x = block(h, a[h], bi)
            total = gv[h, y, x].astype(F32) + whole(d1(h, k), 0) + whole(d1(h, k), 1)
            tf[h, k] = total
            if k < 3:
                tb[h, k] = total.astype(BF16)
            if k == 0:
                for direction in range(2):
                    send(
                        "rs", ("r2",),
                        tb.at[h, 0, :, side_cols(direction)],
                        r2(h).at[direction],
                        along_second(h, direction),
                    )
            if k in (1, 2):
                direction = k - 1
                other = 1 - direction
                send(
                    "rs", ("d2",),
                    tb.at[h, k, :, side_cols(other)],
                    d2(h).at[direction * 2 + other],
                    along_second(h, direction),
                )

    def relay_second():
        arrived(("r2",), land.at[pl.ds(48, 4)])
        for h in range(2):
            for direction in range(2):
                x2[h, direction] = (
                    tf[h, 1 + direction, :, side_cols(direction)]
                    + r2(h)[direction].astype(F32)
                ).astype(BF16)
                send(
                    "rs", ("d2",),
                    x2.at[h, direction],
                    d2(h).at[direction * 2 + direction],
                    along_second(h, direction),
                )

    loaded(("gx",), gx)
    for k in range(4):
        send_far(k)
    tell(0)
    loaded(("gv",), gv)
    send_near(0)
    told(0)
    tell(1)
    told(1)
    tell(2)
    told(2)
    tell(3)
    relay(0)
    send_near(1)
    told(3)
    tell(4)
    relay(1)
    relay(2)
    told(4)
    tell(5)
    send_near(2)
    complete(0)
    told(5)
    tell(6)
    relay(3)
    complete(1)
    told(6)
    tell(7)
    send_near(3)
    complete(2)
    relay_second()
    complete(3)
    for r in range(7, len(rounds)):
        told(r)
        if r + 1 < len(rounds):
            tell(r + 1)
    loaded(("state",), state)

    lanes = jnp.zeros((8, 128), F32)
    arrived(("d2",), land.at[pl.ds(52, 8)])
    for h in range(2):
        total = tf[h, 3] + whole(d2(h), 0) + whole(d2(h), 1)
        tf[h, 3] = total
        square = total * total
        by_row = jnp.sum(square.reshape(-1, 8, half), axis=0)
        for c in range(half // 128):
            lanes = lanes + by_row[:, c * 128 : (c + 1) * 128]

    me = ((iz * n_core + ic) * 4 + iy) * 4 + ix
    parts[me] = jnp.sum(lanes, axis=0, keepdims=True)

    def tell_part(device):
        send("norm", ("norm",), parts.at[me], parts.at[me], device)

    def tell_row(z, i):
        for x in range(4):
            tell_part({"z": z, "core": i // 4, "y": i % 4, "x": x})

    for z in (0, 1, 2, 3, 7, 4, 5, 6):
        @pl.when(z != iz)
        def _():
            for i in range(4 * n_core):
                tell_row(z, i)

    for i in range(n_core):
        for y in range(4):
            for x in range(4):
                if (i, y, x) != (0, 0, 0):
                    tell_part({"core": up(ic, i, n_core), "y": up(iy, y), "x": up(ix, x)})

    n_all = 16 * z_size * n_core
    arrived(("norm",), parts.at[pl.ds(0, n_all - 1)])
    rest = [parts[i] for i in range(n_all)]
    while len(rest) > 1:
        rest = [p + q for p, q in zip(rest[::2], rest[1::2])]
    square_sum = jnp.sum(rest[0], axis=1, keepdims=True)
    limit = 0.5 * math.sqrt(entries)
    factor = jnp.minimum(1.0, limit / jnp.sqrt(square_sum + 1e-06))

    def update(h, side):
        at = cols(h, side)
        clipped = factor * tf[h, 3, :, side_cols(side)]
        new_first = 0.9 * state[1, :, at] + 0.1 * clipped
        new_second = 0.95 * state[2, :, at] + 0.05 * clipped * clipped
        first_hat = new_first * (1.0 / first_bias)
        second_hat = new_second * (1.0 / second_bias)
        master = state[0, :, at]
        new_master = master - 0.01 * (
            first_hat / (jnp.sqrt(second_hat) + 1e-08) + 0.1 * master
        )
        params[iy, ix, :, at] = new_master.astype(BF16)
        w_out[:, at] = new_master
        m_out[:, at] = new_first
        v_out[:, at] = new_second

    def piece(h, ai, bi, side):
        y, x = block(h, ai, bi)
        return params.at[y, x, :, cols(h, side)]

    arrived_from = (0, 3, 1, 2)

    two, four = x2.at[0], x2

    def gather_second(h, direction, side):
        part = piece(h, a[h], b[h], side)
        send("ag", ("g2", direction, side), part, part, along_second(h, direction))

    def forward_second(direction):
        arrived(("g2", direction, direction), two)
        for h in range(2):
            part = piece(h, a[h], up(b[h], step_of[1 - direction]), direction)
            send("ag", ("f2", direction), part, part, along_second(h, direction))

    def gather_first(j, side):
        if j in (1, 2) and side != j - 1:
            arrived(("g2", j - 1, side), two)
        if j == 3:
            arrived(("f2", side), two)
        for h in range(2):
            part = piece(h, a[h], up(b[h], arrived_from[j]), side)
            for direction in range(2):
                send("ag", ("g1", j, side), part, part, along_first(h, direction))

    def forward_first(j, direction):
        arrived(("g1", j, direction), four)
        for h in range(2):
            came_from = up(a[h], step_of[1 - direction])
            part = piece(h, came_from, up(b[h], arrived_from[j]), direction)
            send("ag", ("f1",), part, part, along_first(h, direction))

    for direction in range(2):
        for h in range(2):
            update(h, direction)
            gather_second(h, direction, direction)
    gather_first(0, 0)
    gather_first(0, 1)
    for h in range(2):
        for direction in range(2):
            gather_second(h, direction, 1 - direction)
    forward_second(0)
    gather_first(1, 0)
    forward_second(1)
    gather_first(2, 1)
    gather_first(1, 1)
    gather_first(3, 0)
    gather_first(2, 0)
    forward_first(1, 0)
    gather_first(3, 1)
    forward_first(0, 1)
    forward_first(0, 0)
    forward_first(1, 1)
    forward_first(2, 0)
    forward_first(2, 1)
    forward_first(3, 0)
    forward_first(3, 1)
    all_sent("rs", land)
    all_sent("norm", parts.at[pl.ds(0, n_all - 1)])
    arrived(("f1",), x1)
    all_sent("ag", land)


def write_out(*refs):
    n = (len(refs) - 1) // 2
    sources, targets, sems = refs[:n], refs[n : 2 * n], refs[-1]
    copies = []
    for src, dst in zip(sources, targets):
        parts = [(src.at[i], dst.at[i]) for i in range(4)] if len(src.shape) == 4 else [(src, dst)]
        copies += parts
    made = [
        pltpu.make_async_copy(src, dst, sems.at[i]) for i, (src, dst) in enumerate(copies)
    ]
    for copy in made:
        copy.start()
    for copy in made:
        copy.wait()


def per_device(gradients, master_weights, first_moment, second_moment):
    rows, width = master_weights.shape
    entries = rows * lax.axis_size(DP) * lax.axis_size(SHARD) * width
    half, quarter = width // 2, width // 4
    grads = gradients.reshape(4, 4, rows, width)
    shapes = [((4, 4, rows, width), BF16)] + [((rows, width), F32)] * 3
    hbm = pl.BlockSpec(memory_space=pltpu.HBM)
    vmem = pl.BlockSpec(memory_space=pltpu.VMEM)
    z_size = lax.axis_size("z")
    results = pl.pallas_call(
        lambda *refs: kernel(entries, *refs),
        out_shape=[pltpu.VMEM(*shape) for shape in shapes],
        in_specs=[hbm] * 4,
        out_specs=[vmem] * 4,
        scratch_shapes=[
            pltpu.VMEM((2, 4, rows, half), BF16),
            pltpu.VMEM((2, 4, 4, rows, half), BF16),
            pltpu.VMEM((60, rows, quarter), BF16),
            pltpu.VMEM((2, 4, 2, rows, quarter), BF16),
            pltpu.VMEM((2, 4, rows, half), F32),
            pltpu.VMEM((2, 3, rows, half), BF16),
            pltpu.VMEM((2, 2, rows, quarter), BF16),
            pltpu.VMEM((3, rows, width), F32),
            pltpu.VMEM((16 * z_size * lax.axis_size("core"), 1, 128), F32),
            pltpu.SemaphoreType.DMA((len(LOADED),)),
            pltpu.SemaphoreType.DMA((len(SENT),)),
            pltpu.SemaphoreType.DMA((N_RECEIVED,)),
            pltpu.SemaphoreType.REGULAR((4 + z_size // 2,)),
        ],
        compiler_params=pltpu.CompilerParams(
            collective_id=0, has_side_effects=True, vmem_limit_bytes=VMEM_LIMIT
        ),
    )(grads, master_weights, first_moment, second_moment)
    parameters, new_master, new_first, new_second = pl.pallas_call(
        write_out,
        out_shape=[jax.ShapeDtypeStruct(*shape) for shape in shapes],
        in_specs=[vmem] * 4,
        out_specs=[hbm] * 4,
        scratch_shapes=[pltpu.SemaphoreType.DMA((7,))],
        compiler_params=pltpu.CompilerParams(vmem_limit_bytes=2**20),
    )(*results)
    return (parameters.reshape(16 * rows, width), new_master, new_first, new_second)


def solution(mesh):
    split = Mesh(mesh.devices.reshape(4, 4, 8, 2), ("y", "x", "z", "core"))
    return jax.shard_map(
        per_device,
        mesh=split,
        in_specs=(P(DP, SHARD, None), P(SHARD_DP, None), P(SHARD_DP, None), P(SHARD_DP, None)),
        out_specs=(P(SHARD, None), P(SHARD_DP, None), P(SHARD_DP, None), P(SHARD_DP, None)),
        check_vma=False,
    )
```

```python
import math

import jax
import jax.numpy as jnp
from jax import lax
from jax.experimental import pallas as pl
from jax.experimental.pallas import tpu as pltpu
from jax.sharding import Mesh
from jax.sharding import PartitionSpec as P

DP = ("y", "x")
SHARD = ("z", "core")
SHARD_DP = ("z", "core", "y", "x")
MESH = pl.DeviceIdType.MESH

first_bias = 1.0 - math.exp(100.0 * math.log(0.9))
second_bias = 1.0 - math.exp(100.0 * math.log(0.95))

F32 = jnp.float32
BF16 = jnp.bfloat16
VMEM_LIMIT = 59 * 2**20


def table(*groups):
    keys = []
    for name, *dims in groups:
        index = [()]
        for dim in dims:
            index = [i + (j,) for i in index for j in range(dim)]
        keys += [(name, *i) for i in index]
    return {key: at for at, key in enumerate(keys)}


NORM = table(("norm",))
REDUCE = table(*NORM, ("r1", 4), ("d1", 4), ("r2",), ("d2",))
GATHER = table(*NORM, ("g2", 2, 2), ("f2", 2), ("g1", 4, 2), ("f1",))
RECEIVED = {**REDUCE, **GATHER}
N_RECEIVED = max(len(REDUCE), len(GATHER))
SENT = table(("rs",), ("norm",), ("ag",))
LOADED = table(("gx",), ("gv",), ("state",))


def kernel(
    entries,
    g_hbm, w_hbm, m_hbm, v_hbm,
    params, w_out, m_out, v_out,
    gx, gv, land, x1, tf, tb, x2, state, parts,
    load_sems, send_sems, recv_sems, gossip,
):
    ix, iy = lax.axis_index("x"), lax.axis_index("y")
    iz, ic = lax.axis_index("z"), lax.axis_index("core")
    z_size = lax.axis_size("z")
    n_core = lax.axis_size("core")
    half = g_hbm.shape[3] // 2
    quarter = half // 2

    def up(i, by, n=4):
        return lax.rem(i + by, n)

    first_axis, second_axis = ("x", "y"), ("y", "x")
    a = (ix, iy)
    b = (iy, ix)
    step_of = (1, 3)
    group_by = (2, 1, 3, 0)

    def r1(h, k):
        return land.at[pl.ds((k * 2 + h) * 2, 2)]

    def d1(h, k):
        return land.at[pl.ds(16 + (k * 2 + h) * 4, 4)]

    def r2(h):
        return land.at[pl.ds(48 + h * 2, 2)]

    def d2(h):
        return land.at[pl.ds(52 + h * 4, 4)]

    def whole(ref, direction):
        return jnp.concatenate(
            [ref[direction * 2].astype(F32), ref[direction * 2 + 1].astype(F32)], axis=1
        )

    def cols(h, side=None):
        if side is None:
            return pl.ds(h * half, half)
        return pl.ds(h * half + side * quarter, quarter)

    def side_cols(side):
        return pl.ds(side * quarter, quarter)

    def block(h, ai, bi):
        return (bi, ai) if h == 0 else (ai, bi)

    def near(axis, i, direction):
        return {axis: up(i, step_of[direction])}

    def along_first(h, direction):
        return near(first_axis[h], a[h], direction)

    def along_second(h, direction):
        return near(second_axis[h], b[h], direction)

    def load(key, src, dst):
        pltpu.make_async_copy(src, dst, load_sems.at[LOADED[key]]).start()

    def loaded(key, dst):
        pltpu.make_async_copy(dst, dst, load_sems.at[LOADED[key]]).wait()

    barrier = pltpu.get_barrier_semaphore()
    neighbours = [{"x": up(ix, s)} for s in step_of] + [{"y": up(iy, s)} for s in step_of]
    neighbours += [{"z": up(iz, s, z_size)} for s in (1, z_size - 1)]
    neighbours += [{"core": up(ic, s, n_core)} for s in range(1, n_core)]
    for device in neighbours:
        pl.semaphore_signal(barrier, inc=1, device_id=device, device_id_type=MESH)

    for h in range(2):
        far = up(a[h], 2)
        src = g_hbm.at[:, far, :, cols(h)] if h == 0 else g_hbm.at[far, :, :, cols(h)]
        load(("gx",), src, gx.at[h])
    for h in range(2):
        load(("gv",), g_hbm.at[:, :, :, cols(h)], gv.at[h])
    for i, ref in enumerate((w_hbm, m_hbm, v_hbm)):
        load(("state",), ref, state.at[i])
    pl.semaphore_wait(barrier, len(neighbours))

    links = {
        "x": [{"x": up(ix, s)} for s in step_of],
        "core": [{"core": up(ic, s, n_core)} for s in range(1, n_core)],
        "y": [{"y": up(iy, s)} for s in step_of],
        "z": [{"z": up(iz, s, z_size)} for s in (1, z_size - 1)],
    }
    rounds = ["x", "core", "y", "y"] + ["z"] * (z_size // 2)

    def tell(r):
        for device in links[rounds[r]]:
            pl.semaphore_signal(gossip.at[r], inc=1, device_id=device, device_id_type=MESH)

    def told(r):
        pl.semaphore_wait(gossip.at[r], len(links[rounds[r]]))

    def send(sent, key, src, dst, device):
        pltpu.make_async_remote_copy(
            src_ref=src,
            dst_ref=dst,
            send_sem=send_sems.at[SENT[sent,]],
            recv_sem=recv_sems.at[RECEIVED[key]],
            device_id=device,
            device_id_type=MESH,
        ).start()

    def arrived(key, bytes_of):
        pltpu.make_async_copy(bytes_of, bytes_of, recv_sems.at[RECEIVED[key]]).wait()

    def all_sent(sent, bytes_of):
        pltpu.make_async_copy(bytes_of, bytes_of, send_sems.at[SENT[sent,]]).wait()

    def send_far(k):
        for h in range(2):
            bi = up(b[h], group_by[k])
            for direction in range(2):
                send(
                    "rs", ("r1", k),
                    gx.at[h, bi, :, side_cols(direction)],
                    r1(h, k).at[direction],
                    along_first(h, direction),
                )

    def send_near(k):
        for h in range(2):
            bi = up(b[h], group_by[k])
            for direction in range(2):
                other = 1 - direction
                y, x = block(h, up(a[h], step_of[direction]), bi)
                send(
                    "rs", ("d1", k),
                    gv.at[h, y, x, :, side_cols(other)],
                    d1(h, k).at[direction * 2 + other],
                    along_first(h, direction),
                )

    def relay(k):
        arrived(("r1", k), land.at[pl.ds(k * 4, 4)])
        for h in range(2):
            bi = up(b[h], group_by[k])
            for direction in range(2):
                y, x = block(h, up(a[h], step_of[direction]), bi)
                x1[h, k, direction] = (
                    gv[h, y, x, :, side_cols(direction)].astype(F32)
                    + r1(h, k)[direction].astype(F32)
                ).astype(BF16)
                send(
                    "rs", ("d1", k),
                    x1.at[h, k, direction],
                    d1(h, k).at[direction * 2 + direction],
                    along_first(h, direction),
                )

    def complete(k):
        arrived(("d1", k), land.at[pl.ds(16 + k * 8, 8)])
        for h in range(2):
            bi = up(b[h], group_by[k])
            y, x = block(h, a[h], bi)
            total = gv[h, y, x].astype(F32) + whole(d1(h, k), 0) + whole(d1(h, k), 1)
            tf[h, k] = total
            if k < 3:
                tb[h, k] = total.astype(BF16)
            if k == 0:
                for direction in range(2):
                    send(
                        "rs", ("r2",),
                        tb.at[h, 0, :, side_cols(direction)],
                        r2(h).at[direction],
                        along_second(h, direction),
                    )
            if k in (1, 2):
                direction = k - 1
                other = 1 - direction
                send(
                    "rs", ("d2",),
                    tb.at[h, k, :, side_cols(other)],
                    d2(h).at[direction * 2 + other],
                    along_second(h, direction),
                )

    def relay_second():
        arrived(("r2",), land.at[pl.ds(48, 4)])
        for h in range(2):
            for direction in range(2):
                x2[h, direction] = (
                    tf[h, 1 + direction, :, side_cols(direction)]
                    + r2(h)[direction].astype(F32)
                ).astype(BF16)
                send(
                    "rs", ("d2",),
                    x2.at[h, direction],
                    d2(h).at[direction * 2 + direction],
                    along_second(h, direction),
                )

    loaded(("gx",), gx)
    for k in range(4):
        send_far(k)
    tell(0)
    loaded(("gv",), gv)
    send_near(0)
    told(0)
    tell(1)
    told(1)
    tell(2)
    told(2)
    tell(3)
    relay(0)
    send_near(1)
    told(3)
    tell(4)
    relay(1)
    relay(2)
    told(4)
    tell(5)
    send_near(2)
    complete(0)
    told(5)
    tell(6)
    relay(3)
    complete(1)
    told(6)
    tell(7)
    send_near(3)
    complete(2)
    relay_second()
    complete(3)
    for r in range(7, len(rounds)):
        told(r)
        if r + 1 < len(rounds):
            tell(r + 1)
    loaded(("state",), state)

    lanes = jnp.zeros((8, 128), F32)
    arrived(("d2",), land.at[pl.ds(52, 8)])
    for h in range(2):
        total = tf[h, 3] + whole(d2(h), 0) + whole(d2(h), 1)
        tf[h, 3] = total
        square = total * total
        by_row = jnp.sum(square.reshape(-1, 8, half), axis=0)
        for c in range(half // 128):
            lanes = lanes + by_row[:, c * 128 : (c + 1) * 128]

    me = ((iz * n_core + ic) * 4 + iy) * 4 + ix
    parts[me] = jnp.sum(lanes, axis=0, keepdims=True)

    def tell_part(device):
        send("norm", ("norm",), parts.at[me], parts.at[me], device)

    def tell_row(z, i):
        for x in range(4):
            tell_part({"z": z, "core": i // 4, "y": i % 4, "x": x})

    for z in (0, 1, 2, 3, 7, 4, 5, 6):
        @pl.when(z != iz)
        def _():
            for i in range(4 * n_core):
                tell_row(z, i)

    for i in range(n_core):
        for y in range(4):
            for x in range(4):
                if (i, y, x) != (0, 0, 0):
                    tell_part({"core": up(ic, i, n_core), "y": up(iy, y), "x": up(ix, x)})

    n_all = 16 * z_size * n_core
    arrived(("norm",), parts.at[pl.ds(0, n_all - 1)])
    rest = [parts[i] for i in range(n_all)]
    while len(rest) > 1:
        rest = [p + q for p, q in zip(rest[::2], rest[1::2])]
    square_sum = jnp.sum(rest[0], axis=1, keepdims=True)
    limit = 0.5 * math.sqrt(entries)
    factor = jnp.minimum(1.0, limit / jnp.sqrt(square_sum + 1e-06))

    def adam(h, side):
        at = cols(h, side)
        clipped = factor * tf[h, 3, :, side_cols(side)]
        new_first = 0.9 * state[1, :, at] + 0.1 * clipped
        new_second = 0.95 * state[2, :, at] + 0.05 * clipped * clipped
        first_hat = new_first * (1.0 / first_bias)
        second_hat = new_second * (1.0 / second_bias)
        master = state[0, :, at]
        new_master = master - 0.01 * (
            first_hat / (jnp.sqrt(second_hat) + 1e-08) + 0.1 * master
        )
        return new_master, new_first, new_second

    def update(h, side):
        params[iy, ix, :, cols(h, side)] = adam(h, side)[0].astype(BF16)

    def keep(h, side):
        at = cols(h, side)
        w_out[:, at], m_out[:, at], v_out[:, at] = adam(h, side)

    def piece(h, ai, bi, side):
        y, x = block(h, ai, bi)
        return params.at[y, x, :, cols(h, side)]

    arrived_from = (0, 3, 1, 2)

    two, four = x2.at[0], x2

    def gather_second(h, direction, side):
        part = piece(h, a[h], b[h], side)
        send("ag", ("g2", direction, side), part, part, along_second(h, direction))

    def forward_second(direction):
        arrived(("g2", direction, direction), two)
        for h in range(2):
            part = piece(h, a[h], up(b[h], step_of[1 - direction]), direction)
            send("ag", ("f2", direction), part, part, along_second(h, direction))

    def gather_first(j, side):
        if j in (1, 2) and side != j - 1:
            arrived(("g2", j - 1, side), two)
        if j == 3:
            arrived(("f2", side), two)
        for h in range(2):
            part = piece(h, a[h], up(b[h], arrived_from[j]), side)
            for direction in range(2):
                send("ag", ("g1", j, side), part, part, along_first(h, direction))

    def forward_first(j, direction):
        arrived(("g1", j, direction), four)
        for h in range(2):
            came_from = up(a[h], step_of[1 - direction])
            part = piece(h, came_from, up(b[h], arrived_from[j]), direction)
            send("ag", ("f1",), part, part, along_first(h, direction))

    for direction in range(2):
        for h in range(2):
            update(h, direction)
            gather_second(h, direction, direction)
    gather_first(0, 0)
    gather_first(0, 1)
    for h in range(2):
        for direction in range(2):
            gather_second(h, direction, 1 - direction)
    for h in range(2):
        for side in range(2):
            keep(h, side)
    forward_second(0)
    gather_first(1, 0)
    forward_second(1)
    gather_first(2, 1)
    gather_first(1, 1)
    gather_first(3, 0)
    gather_first(2, 0)
    forward_first(1, 0)
    gather_first(3, 1)
    forward_first(0, 1)
    forward_first(0, 0)
    forward_first(1, 1)
    forward_first(2, 0)
    forward_first(2, 1)
    forward_first(3, 0)
    forward_first(3, 1)
    all_sent("rs", land)
    all_sent("norm", parts.at[pl.ds(0, n_all - 1)])
    arrived(("f1",), x1)
    all_sent("ag", land)


def write_out(*refs):
    n = (len(refs) - 1) // 2
    sources, targets, sems = refs[:n], refs[n : 2 * n], refs[-1]
    copies = []
    for src, dst in zip(sources, targets):
        parts = [(src.at[i], dst.at[i]) for i in range(4)] if len(src.shape) == 4 else [(src, dst)]
        copies += parts
    made = [
        pltpu.make_async_copy(src, dst, sems.at[i]) for i, (src, dst) in enumerate(copies)
    ]
    for copy in made:
        copy.start()
    for copy in made:
        copy.wait()


def per_device(gradients, master_weights, first_moment, second_moment):
    rows, width = master_weights.shape
    entries = rows * lax.axis_size(DP) * lax.axis_size(SHARD) * width
    half, quarter = width // 2, width // 4
    grads = gradients.reshape(4, 4, rows, width)
    shapes = [((4, 4, rows, width), BF16)] + [((rows, width), F32)] * 3
    hbm = pl.BlockSpec(memory_space=pltpu.HBM)
    vmem = pl.BlockSpec(memory_space=pltpu.VMEM)
    z_size = lax.axis_size("z")
    results = pl.pallas_call(
        lambda *refs: kernel(entries, *refs),
        out_shape=[pltpu.VMEM(*shape) for shape in shapes],
        in_specs=[hbm] * 4,
        out_specs=[vmem] * 4,
        scratch_shapes=[
            pltpu.VMEM((2, 4, rows, half), BF16),
            pltpu.VMEM((2, 4, 4, rows, half), BF16),
            pltpu.VMEM((60, rows, quarter), BF16),
            pltpu.VMEM((2, 4, 2, rows, quarter), BF16),
            pltpu.VMEM((2, 4, rows, half), F32),
            pltpu.VMEM((2, 3, rows, half), BF16),
            pltpu.VMEM((2, 2, rows, quarter), BF16),
            pltpu.VMEM((3, rows, width), F32),
            pltpu.VMEM((16 * z_size * lax.axis_size("core"), 1, 128), F32),
            pltpu.SemaphoreType.DMA((len(LOADED),)),
            pltpu.SemaphoreType.DMA((len(SENT),)),
            pltpu.SemaphoreType.DMA((N_RECEIVED,)),
            pltpu.SemaphoreType.REGULAR((4 + z_size // 2,)),
        ],
        compiler_params=pltpu.CompilerParams(
            collective_id=0, has_side_effects=True, vmem_limit_bytes=VMEM_LIMIT
        ),
    )(grads, master_weights, first_moment, second_moment)
    parameters, new_master, new_first, new_second = pl.pallas_call(
        write_out,
        out_shape=[jax.ShapeDtypeStruct(*shape) for shape in shapes],
        in_specs=[vmem] * 4,
        out_specs=[hbm] * 4,
        scratch_shapes=[pltpu.SemaphoreType.DMA((7,))],
        compiler_params=pltpu.CompilerParams(vmem_limit_bytes=2**20),
    )(*results)
    return (parameters.reshape(16 * rows, width), new_master, new_first, new_second)


def solution(mesh):
    split = Mesh(mesh.devices.reshape(4, 4, 8, 2), ("y", "x", "z", "core"))
    return jax.shard_map(
        per_device,
        mesh=split,
        in_specs=(P(DP, SHARD, None), P(SHARD_DP, None), P(SHARD_DP, None), P(SHARD_DP, None)),
        out_specs=(P(SHARD, None), P(SHARD_DP, None), P(SHARD_DP, None), P(SHARD_DP, None)),
        check_vma=False,
    )
```
